32 devices in a mesh: cls: 16 (over z, y, x), rep: 2 (over core).
Axes of the slice: x: 2, y: 2, z: 4, core: 2. Of those that a mesh axis runs over, the one named last changes fastest.
Arguments:
- queries: bfloat16 [2, 32, 768], P('rep', 'cls'), may hold values from -16 to 16
- positives: int32 [2, 32, 4], replicated, may hold values from -1 to 98303, as said below
- label_vectors: bfloat16 [98304, 768], P('cls'), may hold values from -80 to 80
- refresh_slot: int32 [], replicated, may hold values from 0 to 7
- features: bfloat16 [12288, 768], P(('cls', 'rep')), may hold values from -6 to 6
- encoder_weight: bfloat16 [768, 768], replicated, may hold values from -0.21875 to 0.21875
- encoder_gain: float32 [768], replicated, may hold values from 0.1 to 1.9
- free_vectors: bfloat16 [12288, 768], P(('cls', 'rep')), may hold values from -3 to 3
- targets: int32 [12288], replicated, may hold values from 0 to 12287, as said below
Outputs:
- loss: float32 [2, 32], P('rep', 'cls')
- query_grads: bfloat16 [2, 32, 768], P('rep', 'cls')
- refreshed_vectors: bfloat16 [12288, 768], P(('cls', 'rep'))
The draws below stay inside these ranges and needn't reach their ends.
Inputs may be any that keep to these rules, and one draw needn't show every extreme that they name: `positives`: each row holds 1 to 4 label ids in its first places and -1 in the rest; ids may repeat within a row. `targets`: A permutation. Refreshed row t belongs to owner t // 768. The b-th aligned block of 384 entries names exactly 24 rows of every owner, all in the half b % 2 of that owner's 768 rows.
All inputs are finite; a program needn't handle non-finite values.
Results may differ from the reference program's by a relative error of at most 0.0048.
Values may be sent and summed in bfloat16 or wider, within the bound.
A program may use at most 128 MiB of HBM per device.

```python
import jax
import jax.numpy as jnp
from jax import lax

D = 768
LAB_DEV = 6144
SLOTS = 8
POS = 4
Q_DEV = 2
LABELS = 98304
R_DEV = 768
REFRESH = 12288
QG = 32
N_CLS = 16
N_REP = 2


def label_rows(key, row_ids):
    row_base = jax.random.fold_in(key, 11)

    def one_row(row_id):
        return jax.random.normal(jax.random.fold_in(row_base, row_id), (D,), jnp.float32)
    values = jnp.clip(jax.vmap(one_row)(row_ids), -6.0, 6.0)
    return values


def draw_label_vectors(key, part):
    return label_rows(key, jnp.arange(LABELS, dtype=jnp.int32)).astype(jnp.bfloat16)


def draw_queries(key, part):
    total_rows = N_REP * Q_DEV * N_CLS
    spread = 3.0 * D ** (-0.5)
    values = spread * jnp.clip(jax.random.normal(jax.random.fold_in(key, 21), (total_rows, D), jnp.float32), -6.0, 6.0)
    return values.reshape(N_REP, Q_DEV * N_CLS, D).astype(jnp.bfloat16)


def draw_positives(key, part):
    total_rows = N_REP * Q_DEV * N_CLS
    counts = jax.random.randint(jax.random.fold_in(key, 31), (total_rows,), 1, POS + 1)
    counts = counts.at[0].set(POS).at[1].set(1)
    label_ids = jax.random.randint(jax.random.fold_in(key, 32), (total_rows, POS), 0, LABELS)
    places = jnp.arange(POS, dtype=jnp.int32)[None, :]
    filled = jnp.where(places < counts[:, None], label_ids, -1)
    return filled.reshape(N_REP, Q_DEV * N_CLS, POS).astype(jnp.int32)


def draw_targets(key, part):
    half_rows = LAB_DEV // SLOTS // N_REP
    per_owner = half_rows // N_CLS
    key_list = jax.random.split(jax.random.fold_in(key, 41), N_REP * N_CLS)
    shuffled = jax.vmap(lambda one_key: jax.random.permutation(one_key, half_rows))(key_list)
    shuffled = shuffled.reshape(N_REP, N_CLS, N_CLS, per_owner)
    owners = jnp.arange(N_CLS, dtype=jnp.int32)[None, :, None, None]
    halves = jnp.arange(N_REP, dtype=jnp.int32)[:, None, None, None]
    rows_all = owners * (half_rows * N_REP) + halves * half_rows + shuffled
    rows_all = rows_all.transpose(2, 0, 1, 3).reshape(N_CLS * N_REP, N_CLS * per_owner)
    order_keys = jax.random.split(jax.random.fold_in(key, 42), N_CLS * N_REP)
    orders = jax.vmap(lambda one_key: jax.random.permutation(one_key, N_CLS * per_owner))(order_keys)
    rows_all = jnp.take_along_axis(rows_all, orders, axis=1)
    return rows_all.reshape(-1).astype(jnp.int32)


def block_levels(key, extent, cuts, low, top_value):
    def one(dim, shards_of):
        heights = jax.random.uniform(jax.random.fold_in(jax.random.fold_in(key, 6), dim), (shards_of,), jnp.float32, low / len(cuts), top_value / len(cuts))
        return jnp.repeat(jnp.exp(heights), extent[dim] // shards_of).reshape((-1,) + (1,) * (len(extent) - dim - 1))

    factor_of = one(*cuts[0])
    for cut in cuts[1:]:
        factor_of = factor_of * one(*cut)
    return factor_of


def normal_values(key, shape, width, limit, cuts=(), held_as=jnp.bfloat16):
    loudness = block_levels(key, shape, cuts, -0.22, 0.18) if cuts else 1.0
    values = jax.random.normal(key, shape, jnp.float32) * width * loudness
    return jnp.minimum(jnp.maximum(values, -limit), limit).astype(held_as)


def setup_inputs(seed: int = 0) -> dict:
    key_of = jax.random.split(jax.random.key(seed), 10)
    return {
        "queries": draw_queries(jax.random.fold_in(key_of[9], 71), 0),
        "positives": draw_positives(jax.random.fold_in(key_of[9], 71), 0),
        "label_vectors": draw_label_vectors(jax.random.fold_in(key_of[9], 71), 0),
        "refresh_slot": jax.random.randint(key_of[3], (), 0, SLOTS).astype(jnp.int32),
        "features": normal_values(key_of[4], (REFRESH, D), 1.0, 6.0, ((0, 32),)),
        "encoder_weight": normal_values(key_of[5], (D, D), D ** -0.5, 0.21875),
        "encoder_gain": jnp.clip(1.0 + 0.18 * jax.random.normal(key_of[6], (D,), jnp.float32), 0.1, 1.9),
        "free_vectors": normal_values(key_of[7], (REFRESH, D), 0.5, 3.0, ((0, 32),)),
        "targets": draw_targets(jax.random.fold_in(key_of[9], 71), 0),
    }


def reference(queries, positives, label_vectors, refresh_slot, features, encoder_weight, encoder_gain, free_vectors, targets):
    hidden = jnp.dot(features, encoder_weight, preferred_element_type=jnp.float32)
    normed = hidden * lax.rsqrt(lax.optimization_barrier(jnp.mean(hidden * hidden, axis=1, keepdims=True)) + 1e-06) * encoder_gain
    encoded = lax.optimization_barrier(normed.astype(jnp.bfloat16))
    placed = jnp.zeros((REFRESH, D), jnp.bfloat16).at[targets].set(encoded)
    refreshed = (free_vectors.astype(jnp.float32) + placed.astype(jnp.float32)).astype(jnp.bfloat16)
    blocks = label_vectors.reshape(N_CLS, SLOTS, R_DEV, D)
    zero_index = jnp.zeros((), jnp.int32)
    current = lax.dynamic_update_slice(blocks, refreshed.reshape(N_CLS, 1, R_DEV, D), (zero_index, refresh_slot.astype(jnp.int32), zero_index, zero_index)).reshape(LABELS, D)
    block_size = Q_DEV * 32
    query_blocks = queries.reshape(-1, block_size, D)
    positive_blocks = positives.reshape(-1, block_size, POS)

    def one_block(block_pair):
        block_queries, block_ids = block_pair
        logits = lax.dot_general(block_queries, current, (((1,), (1,)), ((), ())), preferred_element_type=jnp.float32)
        maximum = lax.optimization_barrier(jnp.max(logits, axis=1))
        exp_total = lax.optimization_barrier(jnp.sum(jnp.exp(logits - maximum[:, None]), axis=1))
        log_total = maximum + jnp.log(exp_total)
        valid_ids = block_ids >= 0
        safe_ids = jnp.where(valid_ids, block_ids, 0).astype(jnp.int32)
        picked = jnp.take_along_axis(logits, safe_ids, axis=1)
        id_count = lax.optimization_barrier(jnp.sum(valid_ids.astype(jnp.float32), axis=1))
        positive_sum = lax.optimization_barrier(jnp.sum(jnp.where(valid_ids, picked, jnp.zeros_like(picked)), axis=1))
        block_loss = log_total - positive_sum / id_count
        id_weight = jnp.where(valid_ids, jnp.ones_like(picked), jnp.zeros_like(picked)) / id_count[:, None]
        row_index = jnp.broadcast_to(jnp.arange(block_ids.shape[0], dtype=jnp.int32)[:, None], block_ids.shape)
        target_mass = jnp.zeros(logits.shape, jnp.float32).at[row_index, safe_ids].add(id_weight)
        coefficients = (jnp.exp(logits - log_total[:, None]) - target_mass).astype(jnp.bfloat16)
        block_grads = jnp.dot(coefficients, current, preferred_element_type=jnp.float32).astype(jnp.bfloat16)
        return (block_loss, block_grads)
    losses, grads = lax.map(one_block, (query_blocks, positive_blocks))
    return (losses.reshape(N_REP, QG), grads.reshape(N_REP, QG, D), refreshed)
```

```python
import functools

import jax
import jax.numpy as jnp
from jax import lax
from jax.experimental import pallas as pl
from jax.experimental.pallas import tpu as pltpu
from jax.sharding import PartitionSpec as P

SLOTS = 8
NEG = -1e30
STATS = 128
PARTS = 4
NT = (((1,), (1,)), ((), ()))


def to_column(row, eye):
    return jnp.sum(jnp.where(eye, row, 0.0), axis=1, keepdims=True)


def to_row(col, eye):
    return jnp.sum(jnp.where(eye, col, 0.0), axis=0, keepdims=True)


def eye_of(n):
    shape = (n, n)
    return lax.broadcasted_iota(jnp.int32, shape, 0) == lax.broadcasted_iota(jnp.int32, shape, 1)


def each(count, step):
    if count <= 16:
        for i in range(count):
            step(i)
    else:
        lax.fori_loop(0, count, lambda i, carry: (step(i), carry)[1], 0)


def thirds(x):
    f32, bf16 = jnp.float32, jnp.bfloat16
    high = x.astype(bf16).astype(f32)
    rest = x - high
    mid = rest.astype(bf16).astype(f32)
    return high, mid, rest - mid


def step_kernel(
    n_cls,
    n_rep,
    slot_hbm,
    queries_hbm,
    positives_hbm,
    targets_hbm,
    gain_hbm,
    labels_hbm,
    features_hbm,
    weight_hbm,
    free_hbm,
    loss_ref,
    grads_ref,
    refreshed_ref,
    slot_ref,
    positives_ref,
    targets_ref,
    gain_ref,
    labels,
    features,
    weight,
    free,
    free_seats,
    seating,
    fresh_rows,
    id_counts,
    q_slots,
    q_rows,
    out_rows,
    in_rows,
    logits,
    mixed,
    half_out,
    half_in,
    hits_out,
    hits_in,
    shares_out,
    shares_in,
    load_sem,
    q_sem,
    relay_sem,
    row_send,
    row_recv,
    half_sem,
    share_sem,
):
    f32, bf16 = jnp.float32, jnp.bfloat16
    cls = lax.axis_index("cls")
    rep = lax.axis_index("rep")
    partner = 1 - rep
    me = cls * n_rep + rep
    half_rows, width = features.shape
    padded = out_rows.shape[1]
    per_owner = half_rows // n_cls
    query_rows = q_slots.shape[1]
    n_query = q_rows.shape[0]
    own_half = n_query // n_rep
    usable, slot_rows = labels.shape[0], half_rows * n_rep
    lab_rows = usable * n_rep
    seats = n_cls * padded
    mine = rep * n_cls + cls

    barrier = pltpu.get_barrier_semaphore()

    def greet(i):
        pl.semaphore_signal(barrier, inc=1, device_id=(cls ^ (n_cls - 1 - i), rep))

    each(n_cls - 1, greet)
    pl.semaphore_signal(barrier, inc=1, device_id=(cls, partner))

    chunks = usable // slot_rows
    pairs = [
        (features_hbm, features),
        (targets_hbm, targets_ref),
        (weight_hbm, weight),
        (gain_hbm, gain_ref),
        (queries_hbm.at[0], q_slots.at[mine]),
        (slot_hbm, slot_ref),
        (positives_hbm, positives_ref),
        (free_hbm, free),
    ]
    for k in range(chunks):
        start = pl.multiple_of(rep * usable + k * slot_rows, slot_rows)
        pairs.append((labels_hbm.at[pl.ds(start, slot_rows)], labels.at[pl.ds(k * slot_rows, slot_rows)]))
    loads = [pltpu.make_async_copy(a, b, load_sem.at[i]) for i, (a, b) in enumerate(pairs)]
    for copy in loads:
        copy.start()

    row_i = lax.broadcasted_iota(jnp.int32, (half_rows, half_rows), 0)
    col_i = lax.broadcasted_iota(jnp.int32, (half_rows, half_rows), 1)
    eye = row_i == col_i
    loads[1].wait()
    t_row = targets_ref[me].astype(f32)
    t_col = to_column(t_row, eye)
    rank = jnp.sum(jnp.where(t_col < t_row, 1.0, 0.0), axis=0, keepdims=True)
    owner = jnp.floor((rank + 0.5) * (1.0 / per_owner))
    seat_in = (rank - owner * per_owner).astype(jnp.int32)
    place = (owner.astype(jnp.int32) ^ cls) * padded + seat_in
    place_i = lax.broadcasted_iota(jnp.int32, (seats, half_rows), 0)
    pick = jnp.where(place_i == place, 1.0, 0.0).astype(bf16)
    loads[0].wait()
    ordered = jnp.dot(pick, features[...], preferred_element_type=f32).astype(bf16)
    loads[2].wait()
    hidden = jnp.dot(ordered, weight[...], preferred_element_type=f32)
    scale = lax.rsqrt(jnp.mean(hidden * hidden, axis=1, keepdims=True) + 1e-06)
    loads[3].wait()
    encoded = hidden * scale * gain_ref[...].reshape(1, width)
    for k in range(n_cls):
        out_rows[k] = encoded[k * padded : (k + 1) * padded].astype(bf16)
    loads[4].wait()

    pl.semaphore_wait(barrier, n_cls)

    def query_copy(k, slot, many):
        return pltpu.make_async_remote_copy(
            src_ref=q_slots.at[pl.ds(slot, many)],
            dst_ref=q_slots.at[pl.ds(slot, many)],
            send_sem=q_sem.at[0],
            recv_sem=q_sem.at[1],
            device_id=(cls ^ k, rep),
        )

    def row_copy(k, slot, many, part):
        return pltpu.make_async_remote_copy(
            src_ref=out_rows.at[pl.ds(slot, many)],
            dst_ref=in_rows.at[pl.ds(slot, many)],
            send_sem=row_send,
            recv_sem=row_recv.at[part],
            device_id=(cls ^ k, rep),
        )

    def share_copy(k, source, slot, many):
        return pltpu.make_async_remote_copy(
            src_ref=shares_out.at[pl.ds(source, many)],
            dst_ref=shares_in.at[pl.ds(slot, many)],
            send_sem=share_sem.at[0],
            recv_sem=share_sem.at[1],
            device_id=(cls ^ k, rep),
        )

    each(n_cls - 1, lambda i: query_copy(n_cls - 1 - i, mine, 1).start())
    span = n_cls // PARTS
    for part in reversed(range(PARTS)):
        top = (part + 1) * span - 1
        count = span if part else span - 1
        each(count, lambda i, top=top, part=part: row_copy(top - i, top - i, 1, part).start())
    in_rows[0] = out_rows[0]

    my_base = cls * slot_rows + rep * half_rows
    wanted = my_base.astype(f32) + row_i.astype(f32)

    def find(c, acc):
        t_c = targets_ref[c * n_rep + rep].astype(f32)
        return acc + jnp.where(t_c == wanted, (c + 1).astype(f32), 0.0)

    found = lax.fori_loop(0, n_cls, find, jnp.zeros((half_rows, half_rows), f32))
    src_col = jnp.sum(found, axis=1, keepdims=True) - 1.0
    src_row = to_row(src_col, eye)
    before = jnp.where((src_col == src_row) & (col_i < row_i), 1.0, 0.0)
    count_col = jnp.sum(before, axis=1, keepdims=True)
    seat_col = (src_col.astype(jnp.int32) ^ cls) * padded + count_col.astype(jnp.int32)
    seat_row = to_row(seat_col.astype(f32), eye).astype(jnp.int32)
    seat_i = lax.broadcasted_iota(jnp.int32, (half_rows, seats), 1)
    seating[...] = jnp.where(seat_i == seat_col, 1.0, 0.0).astype(bf16)
    turned_i = lax.broadcasted_iota(jnp.int32, (seats, half_rows), 0)
    turned = jnp.where(turned_i == seat_row, 1.0, 0.0).astype(bf16)
    loads[7].wait()
    free_seats[...] = jnp.dot(turned, free[...], preferred_element_type=f32)

    loads[5].wait()
    loads[6].wait()
    n_pos = positives_ref.shape[1]
    eye = eye_of(own_half)
    ids = []
    for p in range(n_pos):
        rows = [positives_ref[r, p : p + 1, :].astype(f32) for r in range(n_rep)]
        ids.append(jnp.concatenate([to_column(row, eye) for row in rows], axis=0).astype(jnp.int32))
    valid = jnp.zeros((n_query, 1), f32)
    for p in range(n_pos):
        valid = valid + jnp.where(ids[p] >= 0, 1.0, 0.0)
    id_counts[...] = jnp.broadcast_to(valid, id_counts.shape)
    slot_start = slot_ref[0] * slot_rows

    def counts_of(label):
        count = jnp.zeros((n_query, label.shape[1]), f32)
        for p in range(n_pos):
            count = count + jnp.where(ids[p] == label, 1.0, 0.0)
        return count

    part_rows = span * padded
    fresh_base = cls * lab_rows + slot_start + rep * half_rows
    fresh_seen, fresh_count = [], []
    for part in range(PARTS):
        at_i = part * part_rows + lax.broadcasted_iota(jnp.int32, (half_rows, part_rows), 1)
        row_f = lax.broadcasted_iota(jnp.int32, (half_rows, part_rows), 0).astype(f32)
        at_row = jnp.sum(jnp.where(at_i == seat_col, row_f + 1.0, 0.0), axis=0, keepdims=True)
        at_row = at_row.astype(jnp.int32)
        fresh_seen.append(at_row > 0)
        fresh_count.append(counts_of(jnp.where(at_row > 0, fresh_base - 1 + at_row, -2)))

    query_copy(1, 0, n_cls - 1).wait_recv()
    side = q_slots.at[pl.ds(rep * n_cls, n_cls)]
    relay = pltpu.make_async_remote_copy(
        src_ref=side,
        dst_ref=side,
        send_sem=relay_sem.at[0],
        recv_sem=relay_sem.at[1],
        device_id=(cls, partner),
    )
    relay.start()
    relay.wait_recv()
    for s in range(n_cls * n_rep):
        q_rows[s * query_rows : (s + 1) * query_rows] = q_slots[s].astype(f32)
    q = q_rows[...].astype(bf16)

    def split(power):
        high = power.astype(bf16)
        return high, (power - high.astype(f32)).astype(bf16)

    def sums(block, power, count):
        exp_sum = jnp.sum(power, axis=1, keepdims=True)
        pos_sum = jnp.sum(count * jnp.where(count > 0.0, block, 0.0), axis=1, keepdims=True)
        return exp_sum, pos_sum

    n = n_query
    peak = jnp.full((n, 1), NEG, f32)
    for k in range(chunks):
        loads[8 + k].wait()
        at = slice(k * slot_rows, (k + 1) * slot_rows)
        block = lax.dot_general(q, labels[at], NT, preferred_element_type=f32)
        fresh = slot_start == rep * usable + k * slot_rows
        block = jnp.where(fresh, NEG, block)
        logits[:, at] = block
        peak = jnp.maximum(peak, jnp.max(block, axis=1, keepdims=True))
    grad = jnp.zeros((n, width), f32)
    hits = jnp.zeros((n, width), f32)
    exp_sum = jnp.zeros((n, 1), f32)
    pos_sum = jnp.zeros((n, 1), f32)
    for k in range(chunks):
        at = slice(k * slot_rows, (k + 1) * slot_rows)
        first = cls * lab_rows + rep * usable + k * slot_rows
        fresh = slot_start == rep * usable + k * slot_rows
        label = first + lax.broadcasted_iota(jnp.int32, (n, slot_rows), 1)
        count = jnp.where(fresh, 0.0, counts_of(label))
        block = logits[:, at]
        power = jnp.exp(block - peak)
        mixed[0:n], mixed[n : 2 * n] = split(power)
        mixed[2 * n : 3 * n] = count.astype(bf16)
        out = jnp.dot(mixed[...], labels[at], preferred_element_type=f32)
        e, s = sums(block, power, count)
        grad = grad + (out[0:n] + out[n : 2 * n])
        hits, exp_sum, pos_sum = hits + out[2 * n : 3 * n], exp_sum + e, pos_sum + s

    for part in [PARTS - 1, *range(PARTS - 1)]:
        low = part * span if part else 1
        row_copy(1, low, (part + 1) * span - low, part).wait_recv()
        at = slice(part * part_rows, (part + 1) * part_rows)
        landed = [in_rows[k].astype(f32) for k in range(part * span, (part + 1) * span)]
        vectors = (free_seats[at] + jnp.concatenate(landed, axis=0)).astype(bf16)
        fresh_rows[at] = vectors
        block = lax.dot_general(q, vectors, NT, preferred_element_type=f32)
        block = jnp.where(fresh_seen[part], block, NEG)
        top = jnp.maximum(peak, jnp.max(block, axis=1, keepdims=True))
        power = jnp.exp(block - top)
        high, rest = split(power)
        count = fresh_count[part]
        out = jnp.dot(
            jnp.concatenate([high, rest, count.astype(bf16)], axis=0), vectors, preferred_element_type=f32
        )
        e, s = sums(block, power, count)
        a = jnp.exp(peak - top)
        grad = grad * a + (out[0:n] + out[n : 2 * n])
        hits, exp_sum, pos_sum = hits + out[2 * n : 3 * n], exp_sum * a + e, pos_sum + s
        peak = top

    lane = lax.broadcasted_iota(jnp.int32, (n, STATS), 1)
    stats = jnp.where(lane == 0, peak, jnp.where(lane == 1, exp_sum, pos_sum))
    for r in range(n_rep):
        at = slice(r * own_half, (r + 1) * own_half)
        half_out[r, :, 0:width] = grad[at]
        half_out[r, :, width:] = stats[at]
        hits_out[r] = hits[at].astype(bf16)
    swaps = []
    for i, (a, b) in enumerate([(half_out, half_in), (hits_out, hits_in)]):
        swap = pltpu.make_async_remote_copy(
            src_ref=a.at[partner],
            dst_ref=b,
            send_sem=half_sem.at[i],
            recv_sem=half_sem.at[2 + i],
            device_id=(cls, partner),
        )
        swap.start()
        swaps.append(swap)
    x, xh = half_out[rep], hits_out[rep].astype(f32)
    some = id_counts[pl.ds(pl.multiple_of(rep * own_half, own_half), own_half), :][:, 0:1]
    for swap in swaps:
        swap.wait_recv()
    y, yh = half_in[...], hits_in[...].astype(f32)
    xs, ys = x[:, width:], y[:, width:]
    m = jnp.maximum(xs[:, 0:1], ys[:, 0:1])
    a, b = jnp.exp(xs[:, 0:1] - m), jnp.exp(ys[:, 0:1] - m)
    exp_sum = xs[:, 1:2] * a + ys[:, 1:2] * b
    pos_sum = xs[:, 2:3] + ys[:, 2:3]
    hits = xh + yh
    inv = 1.0 / exp_sum
    term = x[:, 0:width] * (a * inv) + y[:, 0:width] * (b * inv) - hits * (1.0 / some)
    lane = lax.broadcasted_iota(jnp.int32, (own_half, STATS), 1)
    stats = jnp.zeros((own_half, STATS), f32)
    for i, value in enumerate([m, exp_sum, pos_sum]):
        for j, piece in enumerate(thirds(value)):
            stats = jnp.where(lane == 3 * j + i, piece, stats)
    term, hits, stats = term.astype(bf16), hits.astype(bf16), stats.astype(bf16)
    for c in range(n_cls):
        at = slice(c * query_rows, (c + 1) * query_rows)
        shares_out[c, :, 0:width] = term[at]
        shares_out[c, :, width : 2 * width] = hits[at]
        shares_out[c, :, 2 * width :] = stats[at]

    def send_share(i):
        k = n_cls - 1 - i
        share_copy(k, cls ^ k, k, 1).start()

    each(n_cls - 1, send_share)
    shares_in[0] = shares_out[cls]

    refreshed = jnp.dot(seating[...], fresh_rows[...], preferred_element_type=f32)
    refreshed_ref[...] = refreshed.astype(bf16)
    query_copy(1, 0, n_cls - 1).wait_send()
    row_copy(1, 1, n_cls - 1, 0).wait_send()
    relay.wait_send()
    for swap in swaps:
        swap.wait_send()
    id_count = id_counts[pl.ds(mine * query_rows, query_rows), :][:, 0:1]

    share_copy(1, 0, 1, n_cls - 1).wait_recv()
    stats = shares_in[:, :, 2 * width :].astype(f32)
    stats = stats[:, :, 0:3] + stats[:, :, 3:6] + stats[:, :, 6:9]
    ms, es = stats[:, :, 0:1], stats[:, :, 1:2]
    pos_sum = jnp.sum(stats[:, :, 2:3], axis=0)
    m = jnp.max(ms, axis=0)
    es = es * jnp.exp(ms - m[None])
    exp_sum = jnp.sum(es, axis=0)
    rho = es * (1.0 / exp_sum)[None]
    inv = 1.0 / id_count
    back = (rho - 1.0) * inv[None]
    grad = jnp.zeros((query_rows, width), f32)
    for k in range(n_cls):
        grad = grad + rho[k] * shares_in[k, :, 0:width].astype(f32)
        grad = grad + back[k] * shares_in[k, :, width : 2 * width].astype(f32)
    loss = m + jnp.log(exp_sum) - pos_sum / id_count
    loss_ref[...] = to_row(loss, eye_of(query_rows))
    grads_ref[0] = grad.astype(bf16)
    share_copy(1, 0, 1, n_cls - 1).wait_send()


def pass_on(*refs):
    sem = refs[-1]
    half = len(refs) // 2
    copies = []
    for i, (source, target) in enumerate(zip(refs[:half], refs[half:-1])):
        copy = pltpu.make_async_copy(source, target, sem.at[i])
        copy.start()
        copies.append(copy)
    for copy in copies:
        copy.wait()


def per_device(
    n_cls,
    n_rep,
    queries,
    positives,
    label_vectors,
    refresh_slot,
    features,
    encoder_weight,
    encoder_gain,
    free_vectors,
    targets,
):
    f32, bf16 = jnp.float32, jnp.bfloat16
    total = n_cls * n_rep
    lab_rows, width = label_vectors.shape
    usable = lab_rows // n_rep
    slot_rows = lab_rows // SLOTS
    half_rows = slot_rows // n_rep
    per_owner = half_rows // n_cls
    padded = -(-per_owner // 8) * 8
    query_rows = queries.shape[1]
    n_query = total * query_rows
    own_half = n_query // n_rep
    n_pos = positives.shape[2]
    share = 2 * width + STATS
    vmem = pl.BlockSpec(memory_space=pltpu.VMEM)
    hbm = pl.BlockSpec(memory_space=pl.ANY)
    dma = pltpu.SemaphoreType.DMA
    outs = (
        ((1, query_rows), f32),
        ((1, query_rows, width), bf16),
        ((half_rows, width), bf16),
    )
    results = pl.pallas_call(
        functools.partial(step_kernel, n_cls, n_rep),
        out_shape=tuple(pltpu.VMEM(*out) for out in outs),
        in_specs=[hbm] * 9,
        out_specs=(vmem,) * 3,
        scratch_shapes=[
            pltpu.SMEM((1,), jnp.int32),
            pltpu.VMEM((n_rep, n_pos, own_half), jnp.int32),
            pltpu.VMEM((total, 1, half_rows), jnp.int32),
            pltpu.VMEM((width,), f32),
            pltpu.VMEM((usable, width), bf16),
            pltpu.VMEM((half_rows, width), bf16),
            pltpu.VMEM((width, width), bf16),
            pltpu.VMEM((half_rows, width), bf16),
            pltpu.VMEM((n_cls * padded, width), f32),
            pltpu.VMEM((half_rows, n_cls * padded), bf16),
            pltpu.VMEM((n_cls * padded, width), bf16),
            pltpu.VMEM((n_query, STATS), f32),
            pltpu.VMEM((total, query_rows, width), bf16),
            pltpu.VMEM((n_query, width), f32),
            pltpu.VMEM((n_cls, padded, width), bf16),
            pltpu.VMEM((n_cls, padded, width), bf16),
            pltpu.VMEM((n_query, usable), f32),
            pltpu.VMEM((3 * n_query, slot_rows), bf16),
            pltpu.VMEM((n_rep, own_half, width + STATS), f32),
            pltpu.VMEM((own_half, width + STATS), f32),
            pltpu.VMEM((n_rep, own_half, width), bf16),
            pltpu.VMEM((own_half, width), bf16),
            pltpu.VMEM((n_cls, query_rows, share), bf16),
            pltpu.VMEM((n_cls, query_rows, share), bf16),
            dma((8 + usable // slot_rows,)),
            dma((2,)),
            dma((2,)),
            dma,
            dma((PARTS,)),
            dma((4,)),
            dma((2,)),
        ],
        compiler_params=pltpu.CompilerParams(
            collective_id=0, has_side_effects=True, vmem_limit_bytes=48 * 2**20
        ),
    )(
        refresh_slot.reshape(1),
        queries,
        positives.transpose(0, 2, 1),
        targets.reshape(total, 1, half_rows),
        encoder_gain,
        label_vectors,
        features,
        encoder_weight,
        free_vectors,
    )
    return pl.pallas_call(
        pass_on,
        out_shape=tuple(jax.ShapeDtypeStruct(*out) for out in outs),
        in_specs=[vmem] * 3,
        out_specs=(hbm,) * 3,
        scratch_shapes=[dma((3,))],
    )(*results)


def solution(mesh):
    placed = (
        P("rep", "cls", None),
        P(),
        P("cls", None),
        P(),
        P(("cls", "rep"), None),
        P(),
        P(),
        P(("cls", "rep"), None),
        P(),
    )
    return jax.shard_map(
        functools.partial(per_device, mesh.shape["cls"], mesh.shape["rep"]),
        mesh=mesh,
        in_specs=placed,
        out_specs=(P("rep", "cls"), P("rep", "cls", None), P(("cls", "rep"), None)),
        check_vma=False,
    )
```

```python
import functools

import jax
import jax.numpy as jnp
from jax import lax
from jax.experimental import pallas as pl
from jax.experimental.pallas import tpu as pltpu
from jax.sharding import PartitionSpec as P

SLOTS = 8
NEG = -1e30
STATS = 128
PARTS = 4
NT = (((1,), (1,)), ((), ()))


def to_column(row, eye):
    return jnp.sum(jnp.where(eye, row, 0.0), axis=1, keepdims=True)


def to_row(col, eye):
    return jnp.sum(jnp.where(eye, col, 0.0), axis=0, keepdims=True)


def eye_of(n):
    shape = (n, n)
    return lax.broadcasted_iota(jnp.int32, shape, 0) == lax.broadcasted_iota(jnp.int32, shape, 1)


def each(count, step):
    if count <= 16:
        for i in range(count):
            step(i)
    else:
        lax.fori_loop(0, count, lambda i, carry: (step(i), carry)[1], 0)


def thirds(x):
    f32, bf16 = jnp.float32, jnp.bfloat16
    high = x.astype(bf16).astype(f32)
    rest = x - high
    mid = rest.astype(bf16).astype(f32)
    return high, mid, rest - mid


def step_kernel(
    n_cls,
    n_rep,
    slot_hbm,
    queries_hbm,
    positives_hbm,
    targets_hbm,
    gain_hbm,
    labels_hbm,
    features_hbm,
    weight_hbm,
    free_hbm,
    loss_ref,
    grads_ref,
    refreshed_ref,
    slot_ref,
    positives_ref,
    targets_ref,
    gain_ref,
    labels,
    features,
    weight,
    free,
    free_seats,
    seating,
    fresh_rows,
    id_counts,
    q_slots,
    q_rows,
    out_rows,
    in_rows,
    logits,
    mixed,
    half_out,
    half_in,
    hits_out,
    hits_in,
    shares_out,
    shares_in,
    load_sem,
    q_sem,
    relay_sem,
    row_send,
    row_recv,
    half_sem,
    share_sem,
):
    f32, bf16 = jnp.float32, jnp.bfloat16
    cls = lax.axis_index("cls")
    rep = lax.axis_index("rep")
    partner = 1 - rep
    me = cls * n_rep + rep
    half_rows, width = features.shape
    padded = out_rows.shape[1]
    per_owner = half_rows // n_cls
    query_rows = q_slots.shape[1]
    n_query = q_rows.shape[0]
    own_half = n_query // n_rep
    usable, slot_rows = labels.shape[0], half_rows * n_rep
    lab_rows = usable * n_rep
    seats = n_cls * padded
    mine = rep * n_cls + cls

    barrier = pltpu.get_barrier_semaphore()

    def greet(i):
        pl.semaphore_signal(barrier, inc=1, device_id=(cls ^ (n_cls - 1 - i), rep))

    each(n_cls - 1, greet)
    pl.semaphore_signal(barrier, inc=1, device_id=(cls, partner))

    chunks = usable // slot_rows
    pairs = [
        (features_hbm, features),
        (targets_hbm, targets_ref),
        (weight_hbm, weight),
        (gain_hbm, gain_ref),
        (queries_hbm.at[0], q_slots.at[mine]),
        (slot_hbm, slot_ref),
        (positives_hbm, positives_ref),
        (free_hbm, free),
    ]
    for k in range(chunks):
        start = pl.multiple_of(rep * usable + k * slot_rows, slot_rows)
        pairs.append((labels_hbm.at[pl.ds(start, slot_rows)], labels.at[pl.ds(k * slot_rows, slot_rows)]))
    loads = [pltpu.make_async_copy(a, b, load_sem.at[i]) for i, (a, b) in enumerate(pairs)]
    for copy in loads:
        copy.start()

    row_i = lax.broadcasted_iota(jnp.int32, (half_rows, half_rows), 0)
    col_i = lax.broadcasted_iota(jnp.int32, (half_rows, half_rows), 1)
    eye = row_i == col_i
    loads[1].wait()
    t_row = targets_ref[me].astype(f32)
    t_col = to_column(t_row, eye)
    rank = jnp.sum(jnp.where(t_col < t_row, 1.0, 0.0), axis=0, keepdims=True)
    owner = jnp.floor((rank + 0.5) * (1.0 / per_owner))
    seat_in = (rank - owner * per_owner).astype(jnp.int32)
    place = (owner.astype(jnp.int32) ^ cls) * padded + seat_in
    place_i = lax.broadcasted_iota(jnp.int32, (seats, half_rows), 0)
    pick = jnp.where(place_i == place, 1.0, 0.0).astype(bf16)
    loads[0].wait()
    ordered = jnp.dot(pick, features[...], preferred_element_type=f32).astype(bf16)
    loads[2].wait()
    hidden = jnp.dot(ordered, weight[...], preferred_element_type=f32)
    scale = lax.rsqrt(jnp.mean(hidden * hidden, axis=1, keepdims=True) + 1e-06)
    loads[3].wait()
    encoded = hidden * scale * gain_ref[...].reshape(1, width)
    for k in range(n_cls):
        out_rows[k] = encoded[k * padded : (k + 1) * padded].astype(bf16)
    loads[4].wait()

    pl.semaphore_wait(barrier, n_cls)

    def query_copy(k, slot, many):
        return pltpu.make_async_remote_copy(
            src_ref=q_slots.at[pl.ds(slot, many)],
            dst_ref=q_slots.at[pl.ds(slot, many)],
            send_sem=q_sem.at[0],
            recv_sem=q_sem.at[1],
            device_id=(cls ^ k, rep),
        )

    def row_copy(k, slot, many, part):
        return pltpu.make_async_remote_copy(
            src_ref=out_rows.at[pl.ds(slot, many)],
            dst_ref=in_rows.at[pl.ds(slot, many)],
            send_sem=row_send,
            recv_sem=row_recv.at[part],
            device_id=(cls ^ k, rep),
        )

    def share_copy(k, source, slot, many):
        return pltpu.make_async_remote_copy(
            src_ref=shares_out.at[pl.ds(source, many)],
            dst_ref=shares_in.at[pl.ds(slot, many)],
            send_sem=share_sem.at[0],
            recv_sem=share_sem.at[1],
            device_id=(cls ^ k, rep),
        )

    each(n_cls - 1, lambda i: query_copy(n_cls - 1 - i, mine, 1).start())
    query_copy(1, 0, n_cls - 1).wait_send()
    span = n_cls // PARTS
    for part in reversed(range(PARTS)):
        top = (part + 1) * span - 1
        count = span if part else span - 1
        each(count, lambda i, top=top, part=part: row_copy(top - i, top - i, 1, part).start())
    in_rows[0] = out_rows[0]

    my_base = cls * slot_rows + rep * half_rows
    wanted = my_base.astype(f32) + row_i.astype(f32)

    def find(c, acc):
        t_c = targets_ref[c * n_rep + rep].astype(f32)
        return acc + jnp.where(t_c == wanted, (c + 1).astype(f32), 0.0)

    found = lax.fori_loop(0, n_cls, find, jnp.zeros((half_rows, half_rows), f32))
    src_col = jnp.sum(found, axis=1, keepdims=True) - 1.0
    src_row = to_row(src_col, eye)
    before = jnp.where((src_col == src_row) & (col_i < row_i), 1.0, 0.0)
    count_col = jnp.sum(before, axis=1, keepdims=True)
    seat_col = (src_col.astype(jnp.int32) ^ cls) * padded + count_col.astype(jnp.int32)
    seat_row = to_row(seat_col.astype(f32), eye).astype(jnp.int32)
    seat_i = lax.broadcasted_iota(jnp.int32, (half_rows, seats), 1)
    seating[...] = jnp.where(seat_i == seat_col, 1.0, 0.0).astype(bf16)
    turned_i = lax.broadcasted_iota(jnp.int32, (seats, half_rows), 0)
    turned = jnp.where(turned_i == seat_row, 1.0, 0.0).astype(bf16)
    loads[7].wait()
    free_seats[...] = jnp.dot(turned, free[...], preferred_element_type=f32)

    loads[5].wait()
    loads[6].wait()
    n_pos = positives_ref.shape[1]
    eye = eye_of(own_half)
    ids = []
    for p in range(n_pos):
        rows = [positives_ref[r, p : p + 1, :].astype(f32) for r in range(n_rep)]
        ids.append(jnp.concatenate([to_column(row, eye) for row in rows], axis=0).astype(jnp.int32))
    valid = jnp.zeros((n_query, 1), f32)
    for p in range(n_pos):
        valid = valid + jnp.where(ids[p] >= 0, 1.0, 0.0)
    id_counts[...] = jnp.broadcast_to(valid, id_counts.shape)
    slot_start = slot_ref[0] * slot_rows

    def counts_of(label):
        count = jnp.zeros((n_query, label.shape[1]), f32)
        for p in range(n_pos):
            count = count + jnp.where(ids[p] == label, 1.0, 0.0)
        return count

    part_rows = span * padded
    fresh_base = cls * lab_rows + slot_start + rep * half_rows
    fresh_seen, fresh_count = [], []
    for part in range(PARTS):
        at_i = part * part_rows + lax.broadcasted_iota(jnp.int32, (half_rows, part_rows), 1)
        row_f = lax.broadcasted_iota(jnp.int32, (half_rows, part_rows), 0).astype(f32)
        at_row = jnp.sum(jnp.where(at_i == seat_col, row_f + 1.0, 0.0), axis=0, keepdims=True)
        at_row = at_row.astype(jnp.int32)
        fresh_seen.append(at_row > 0)
        fresh_count.append(counts_of(jnp.where(at_row > 0, fresh_base - 1 + at_row, -2)))

    query_copy(1, 0, n_cls - 1).wait_recv()
    side = q_slots.at[pl.ds(rep * n_cls, n_cls)]
    relay = pltpu.make_async_remote_copy(
        src_ref=side,
        dst_ref=side,
        send_sem=relay_sem.at[0],
        recv_sem=relay_sem.at[1],
        device_id=(cls, partner),
    )
    relay.start()
    relay.wait_recv()
    for s in range(n_cls * n_rep):
        q_rows[s * query_rows : (s + 1) * query_rows] = q_slots[s].astype(f32)
    q = q_rows[...].astype(bf16)

    def split(power):
        high = power.astype(bf16)
        return high, (power - high.astype(f32)).astype(bf16)

    def sums(block, power, count):
        exp_sum = jnp.sum(power, axis=1, keepdims=True)
        pos_sum = jnp.sum(count * jnp.where(count > 0.0, block, 0.0), axis=1, keepdims=True)
        return exp_sum, pos_sum

    n = n_query
    peak = jnp.full((n, 1), NEG, f32)
    for k in range(chunks):
        loads[8 + k].wait()
        at = slice(k * slot_rows, (k + 1) * slot_rows)
        block = lax.dot_general(q, labels[at], NT, preferred_element_type=f32)
        fresh = slot_start == rep * usable + k * slot_rows
        block = jnp.where(fresh, NEG, block)
        logits[:, at] = block
        peak = jnp.maximum(peak, jnp.max(block, axis=1, keepdims=True))
    grad = jnp.zeros((n, width), f32)
    hits = jnp.zeros((n, width), f32)
    exp_sum = jnp.zeros((n, 1), f32)
    pos_sum = jnp.zeros((n, 1), f32)
    for k in range(chunks):
        at = slice(k * slot_rows, (k + 1) * slot_rows)
        first = cls * lab_rows + rep * usable + k * slot_rows
        fresh = slot_start == rep * usable + k * slot_rows
        label = first + lax.broadcasted_iota(jnp.int32, (n, slot_rows), 1)
        count = jnp.where(fresh, 0.0, counts_of(label))
        block = logits[:, at]
        power = jnp.exp(block - peak)
        mixed[0:n], mixed[n : 2 * n] = split(power)
        mixed[2 * n : 3 * n] = count.astype(bf16)
        out = jnp.dot(mixed[...], labels[at], preferred_element_type=f32)
        e, s = sums(block, power, count)
        grad = grad + (out[0:n] + out[n : 2 * n])
        hits, exp_sum, pos_sum = hits + out[2 * n : 3 * n], exp_sum + e, pos_sum + s

    for part in [PARTS - 1, *range(PARTS - 1)]:
        low = part * span if part else 1
        row_copy(1, low, (part + 1) * span - low, part).wait_recv()
        at = slice(part * part_rows, (part + 1) * part_rows)
        landed = [in_rows[k].astype(f32) for k in range(part * span, (part + 1) * span)]
        vectors = (free_seats[at] + jnp.concatenate(landed, axis=0)).astype(bf16)
        fresh_rows[at] = vectors
        block = lax.dot_general(q, vectors, NT, preferred_element_type=f32)
        block = jnp.where(fresh_seen[part], block, NEG)
        top = jnp.maximum(peak, jnp.max(block, axis=1, keepdims=True))
        power = jnp.exp(block - top)
        high, rest = split(power)
        count = fresh_count[part]
        out = jnp.dot(
            jnp.concatenate([high, rest, count.astype(bf16)], axis=0), vectors, preferred_element_type=f32
        )
        e, s = sums(block, power, count)
        a = jnp.exp(peak - top)
        grad = grad * a + (out[0:n] + out[n : 2 * n])
        hits, exp_sum, pos_sum = hits + out[2 * n : 3 * n], exp_sum * a + e, pos_sum + s
        peak = top

    lane = lax.broadcasted_iota(jnp.int32, (n, STATS), 1)
    stats = jnp.where(lane == 0, peak, jnp.where(lane == 1, exp_sum, pos_sum))
    for r in range(n_rep):
        at = slice(r * own_half, (r + 1) * own_half)
        half_out[r, :, 0:width] = grad[at]
        half_out[r, :, width:] = stats[at]
        hits_out[r] = hits[at].astype(bf16)
    swaps = []
    for i, (a, b) in enumerate([(half_out, half_in), (hits_out, hits_in)]):
        swap = pltpu.make_async_remote_copy(
            src_ref=a.at[partner],
            dst_ref=b,
            send_sem=half_sem.at[i],
            recv_sem=half_sem.at[2 + i],
            device_id=(cls, partner),
        )
        swap.start()
        swaps.append(swap)
    x, xh = half_out[rep], hits_out[rep].astype(f32)
    some = id_counts[pl.ds(pl.multiple_of(rep * own_half, own_half), own_half), :][:, 0:1]
    for swap in swaps:
        swap.wait_recv()
    y, yh = half_in[...], hits_in[...].astype(f32)
    xs, ys = x[:, width:], y[:, width:]
    m = jnp.maximum(xs[:, 0:1], ys[:, 0:1])
    a, b = jnp.exp(xs[:, 0:1] - m), jnp.exp(ys[:, 0:1] - m)
    exp_sum = xs[:, 1:2] * a + ys[:, 1:2] * b
    pos_sum = xs[:, 2:3] + ys[:, 2:3]
    hits = xh + yh
    inv = 1.0 / exp_sum
    term = x[:, 0:width] * (a * inv) + y[:, 0:width] * (b * inv) - hits * (1.0 / some)
    lane = lax.broadcasted_iota(jnp.int32, (own_half, STATS), 1)
    stats = jnp.zeros((own_half, STATS), f32)
    for i, value in enumerate([m, exp_sum, pos_sum]):
        for j, piece in enumerate(thirds(value)):
            stats = jnp.where(lane == 3 * j + i, piece, stats)
    term, hits, stats = term.astype(bf16), hits.astype(bf16), stats.astype(bf16)
    for c in range(n_cls):
        at = slice(c * query_rows, (c + 1) * query_rows)
        shares_out[c, :, 0:width] = term[at]
        shares_out[c, :, width : 2 * width] = hits[at]
        shares_out[c, :, 2 * width :] = stats[at]

    def send_share(i):
        k = n_cls - 1 - i
        share_copy(k, cls ^ k, k, 1).start()

    each(n_cls - 1, send_share)
    shares_in[0] = shares_out[cls]

    refreshed = jnp.dot(seating[...], fresh_rows[...], preferred_element_type=f32)
    refreshed_ref[...] = refreshed.astype(bf16)
    row_copy(1, 1, n_cls - 1, 0).wait_send()
    relay.wait_send()
    for swap in swaps:
        swap.wait_send()
    id_count = id_counts[pl.ds(mine * query_rows, query_rows), :][:, 0:1]

    share_copy(1, 0, 1, n_cls - 1).wait_recv()
    stats = shares_in[:, :, 2 * width :].astype(f32)
    stats = stats[:, :, 0:3] + stats[:, :, 3:6] + stats[:, :, 6:9]
    ms, es = stats[:, :, 0:1], stats[:, :, 1:2]
    pos_sum = jnp.sum(stats[:, :, 2:3], axis=0)
    m = jnp.max(ms, axis=0)
    es = es * jnp.exp(ms - m[None])
    exp_sum = jnp.sum(es, axis=0)
    rho = es * (1.0 / exp_sum)[None]
    inv = 1.0 / id_count
    back = (rho - 1.0) * inv[None]
    grad = jnp.zeros((query_rows, width), f32)
    for k in range(n_cls):
        grad = grad + rho[k] * shares_in[k, :, 0:width].astype(f32)
        grad = grad + back[k] * shares_in[k, :, width : 2 * width].astype(f32)
    loss = m + jnp.log(exp_sum) - pos_sum / id_count
    loss_ref[...] = to_row(loss, eye_of(query_rows))
    grads_ref[0] = grad.astype(bf16)
    share_copy(1, 0, 1, n_cls - 1).wait_send()


def pass_on(*refs):
    sem = refs[-1]
    half = len(refs) // 2
    copies = []
    for i, (source, target) in enumerate(zip(refs[:half], refs[half:-1])):
        copy = pltpu.make_async_copy(source, target, sem.at[i])
        copy.start()
        copies.append(copy)
    for copy in copies:
        copy.wait()


def per_device(
    n_cls,
    n_rep,
    queries,
    positives,
    label_vectors,
    refresh_slot,
    features,
    encoder_weight,
    encoder_gain,
    free_vectors,
    targets,
):
    f32, bf16 = jnp.float32, jnp.bfloat16
    total = n_cls * n_rep
    lab_rows, width = label_vectors.shape
    usable = lab_rows // n_rep
    slot_rows = lab_rows // SLOTS
    half_rows = slot_rows // n_rep
    per_owner = half_rows // n_cls
    padded = -(-per_owner // 8) * 8
    query_rows = queries.shape[1]
    n_query = total * query_rows
    own_half = n_query // n_rep
    n_pos = positives.shape[2]
    share = 2 * width + STATS
    vmem = pl.BlockSpec(memory_space=pltpu.VMEM)
    hbm = pl.BlockSpec(memory_space=pltpu.HBM)
    dma = pltpu.SemaphoreType.DMA
    outs = (
        ((1, query_rows), f32),
        ((1, query_rows, width), bf16),
        ((half_rows, width), bf16),
    )
    results = pl.pallas_call(
        functools.partial(step_kernel, n_cls, n_rep),
        out_shape=tuple(pltpu.VMEM(*out) for out in outs),
        in_specs=[hbm] * 9,
        out_specs=(vmem,) * 3,
        scratch_shapes=[
            pltpu.SMEM((1,), jnp.int32),
            pltpu.VMEM((n_rep, n_pos, own_half), jnp.int32),
            pltpu.VMEM((total, 1, half_rows), jnp.int32),
            pltpu.VMEM((width,), f32),
            pltpu.VMEM((usable, width), bf16),
            pltpu.VMEM((half_rows, width), bf16),
            pltpu.VMEM((width, width), bf16),
            pltpu.VMEM((half_rows, width), bf16),
            pltpu.VMEM((n_cls * padded, width), f32),
            pltpu.VMEM((half_rows, n_cls * padded), bf16),
            pltpu.VMEM((n_cls * padded, width), bf16),
            pltpu.VMEM((n_query, STATS), f32),
            pltpu.VMEM((total, query_rows, width), bf16),
            pltpu.VMEM((n_query, width), f32),
            pltpu.VMEM((n_cls, padded, width), bf16),
            pltpu.VMEM((n_cls, padded, width), bf16),
            pltpu.VMEM((n_query, usable), f32),
            pltpu.VMEM((3 * n_query, slot_rows), bf16),
            pltpu.VMEM((n_rep, own_half, width + STATS), f32),
            pltpu.VMEM((own_half, width + STATS), f32),
            pltpu.VMEM((n_rep, own_half, width), bf16),
            pltpu.VMEM((own_half, width), bf16),
            pltpu.VMEM((n_cls, query_rows, share), bf16),
            pltpu.VMEM((n_cls, query_rows, share), bf16),
            dma((8 + usable // slot_rows,)),
            dma((2,)),
            dma((2,)),
            dma,
            dma((PARTS,)),
            dma((4,)),
            dma((2,)),
        ],
        compiler_params=pltpu.CompilerParams(
            collective_id=0, has_side_effects=True, vmem_limit_bytes=48 * 2**20
        ),
    )(
        refresh_slot.reshape(1),
        *[
            pltpu.with_memory_space_constraint(x, pltpu.HBM)
            for x in (
                queries,
                positives.transpose(0, 2, 1),
                targets.reshape(total, 1, half_rows),
                encoder_gain,
                label_vectors,
                features,
                encoder_weight,
                free_vectors,
            )
        ]
    )
    return pl.pallas_call(
        pass_on,
        out_shape=tuple(jax.ShapeDtypeStruct(*out) for out in outs),
        in_specs=[vmem] * 3,
        out_specs=(hbm,) * 3,
        scratch_shapes=[dma((3,))],
    )(*[pltpu.with_memory_space_constraint(x, pltpu.VMEM) for x in results])


def solution(mesh):
    placed = (
        P("rep", "cls", None),
        P(),
        P("cls", None),
        P(),
        P(("cls", "rep"), None),
        P(),
        P(),
        P(("cls", "rep"), None),
        P(),
    )
    return jax.shard_map(
        functools.partial(per_device, mesh.shape["cls"], mesh.shape["rep"]),
        mesh=mesh,
        in_specs=placed,
        out_specs=(P("rep", "cls"), P("rep", "cls", None), P(("cls", "rep"), None)),
        check_vma=False,
    )
```

```python
import functools

import jax
import jax.numpy as jnp
from jax import lax
from jax.experimental import pallas as pl
from jax.experimental.pallas import tpu as pltpu
from jax.sharding import PartitionSpec as P

SLOTS = 8
NEG = -1e30
STATS = 128
PARTS = 4
NT = (((1,), (1,)), ((), ()))


def to_column(row, eye):
    return jnp.sum(jnp.where(eye, row, 0.0), axis=1, keepdims=True)


def to_row(col, eye):
    return jnp.sum(jnp.where(eye, col, 0.0), axis=0, keepdims=True)


def eye_of(n):
    shape = (n, n)
    return lax.broadcasted_iota(jnp.int32, shape, 0) == lax.broadcasted_iota(jnp.int32, shape, 1)


def each(count, step):
    if count <= 16:
        for i in range(count):
            step(i)
    else:
        lax.fori_loop(0, count, lambda i, carry: (step(i), carry)[1], 0)


def thirds(x):
    f32, bf16 = jnp.float32, jnp.bfloat16
    high = x.astype(bf16).astype(f32)
    rest = x - high
    mid = rest.astype(bf16).astype(f32)
    return high, mid, rest - mid


def step_kernel(
    n_cls,
    n_rep,
    slot_hbm,
    queries_hbm,
    positives_hbm,
    targets_hbm,
    gain_hbm,
    labels_hbm,
    features_hbm,
    weight_hbm,
    free_hbm,
    loss_ref,
    grads_ref,
    refreshed_ref,
    slot_ref,
    positives_ref,
    targets_ref,
    gain_ref,
    labels,
    turned_labels,
    features,
    weight,
    free,
    free_seats,
    seating,
    fresh_rows,
    fresh_seen,
    fresh_count,
    id_counts,
    q_slots,
    q_rows,
    out_rows,
    in_rows,
    logits,
    mixed,
    half_out,
    half_in,
    hits_out,
    hits_in,
    shares_out,
    shares_in,
    load_sem,
    q_sem,
    relay_sem,
    row_send,
    row_recv,
    half_sem,
    share_sem,
):
    f32, bf16 = jnp.float32, jnp.bfloat16
    cls = lax.axis_index("cls")
    rep = lax.axis_index("rep")
    partner = 1 - rep
    me = cls * n_rep + rep
    half_rows, width = features.shape
    padded = out_rows.shape[1]
    per_owner = half_rows // n_cls
    query_rows = q_slots.shape[1]
    n_query = q_rows.shape[0]
    own_half = n_query // n_rep
    usable, slot_rows = labels.shape[0], half_rows * n_rep
    lab_rows = usable * n_rep
    seats = n_cls * padded
    mine = rep * n_cls + cls
    span = n_cls // PARTS
    plane = cls // span
    inner = (plane > 0) & (plane < PARTS - 1)

    def seat_of(owner):
        return (owner ^ cls) * padded

    barrier = pltpu.get_barrier_semaphore()

    def greet(i):
        pl.semaphore_signal(barrier, inc=1, device_id=(cls ^ (n_cls - 1 - i), rep))

    each(n_cls - 1, greet)
    pl.semaphore_signal(barrier, inc=1, device_id=(cls, partner))

    chunks = usable // slot_rows
    pairs = [
        (features_hbm, features),
        (targets_hbm, targets_ref),
        (weight_hbm, weight),
        (gain_hbm, gain_ref),
        (queries_hbm.at[0], q_slots.at[mine]),
        (slot_hbm, slot_ref),
        (positives_hbm, positives_ref),
        (free_hbm, free),
    ]
    for k in range(chunks):
        start = pl.multiple_of(rep * usable + k * slot_rows, slot_rows)
        pairs.append((labels_hbm.at[pl.ds(start, slot_rows)], labels.at[pl.ds(k * slot_rows, slot_rows)]))
    loads = [pltpu.make_async_copy(a, b, load_sem.at[i]) for i, (a, b) in enumerate(pairs)]
    for copy in loads:
        copy.start()

    row_i = lax.broadcasted_iota(jnp.int32, (half_rows, half_rows), 0)
    col_i = lax.broadcasted_iota(jnp.int32, (half_rows, half_rows), 1)
    eye = row_i == col_i
    loads[1].wait()
    t_row = targets_ref[me].astype(f32)
    t_col = to_column(t_row, eye)
    rank = jnp.sum(jnp.where(t_col < t_row, 1.0, 0.0), axis=0, keepdims=True)
    owner = jnp.floor((rank + 0.5) * (1.0 / per_owner))
    seat_in = (rank - owner * per_owner).astype(jnp.int32)
    place = seat_of(owner.astype(jnp.int32)) + seat_in
    part_rows = span * padded

    def encode(low, high):
        rows = (high - low) * padded
        place_i = low * padded + lax.broadcasted_iota(jnp.int32, (rows, half_rows), 0)
        pick = jnp.where(place_i == place, 1.0, 0.0).astype(bf16)
        ordered = jnp.dot(pick, features[...], preferred_element_type=f32).astype(bf16)
        hidden = jnp.dot(ordered, weight[...], preferred_element_type=f32)
        scale = lax.rsqrt(jnp.mean(hidden * hidden, axis=1, keepdims=True) + 1e-06)
        encoded = hidden * scale * gain_ref[...].reshape(1, width)
        for k in range(low, high):
            out_rows[k] = encoded[(k - low) * padded : (k - low + 1) * padded].astype(bf16)

    loads[0].wait()
    loads[2].wait()
    loads[3].wait()
    encode(n_cls // 2, n_cls)
    loads[4].wait()

    pl.semaphore_wait(barrier, n_cls)

    def query_copy(k, slot, many):
        return pltpu.make_async_remote_copy(
            src_ref=q_slots.at[pl.ds(slot, many)],
            dst_ref=q_slots.at[pl.ds(slot, many)],
            send_sem=q_sem.at[0],
            recv_sem=q_sem.at[1],
            device_id=(cls ^ k, rep),
        )

    def row_copy(slot, many, part):
        return pltpu.make_async_remote_copy(
            src_ref=out_rows.at[pl.ds(slot, many)],
            dst_ref=in_rows.at[pl.ds(slot, many)],
            send_sem=row_send,
            recv_sem=row_recv.at[part],
            device_id=(cls ^ slot, rep),
        )

    def share_copy(k, source, slot, many):
        return pltpu.make_async_remote_copy(
            src_ref=shares_out.at[pl.ds(source, many)],
            dst_ref=shares_in.at[pl.ds(slot, many)],
            send_sem=share_sem.at[0],
            recv_sem=share_sem.at[1],
            device_id=(cls ^ k, rep),
        )

    def send_rows(part):
        top = (part + 1) * span - 1
        each(span if part else span - 1, lambda i: row_copy(top - i, 1, part).start())

    each(n_cls - 1, lambda i: query_copy(i + 1, mine, 1).start())
    pl.when(inner)(lambda: send_rows(2))
    encode(0, n_cls // 2)

    @pl.when(jnp.logical_not(inner))
    def _():
        query_copy(1, 0, n_cls - 1).wait_send()
        for part in (3, 2, 1, 0):
            send_rows(part)

    @pl.when(inner)
    def _():
        for part in (1, 0, 3):
            send_rows(part)

    in_rows[0] = out_rows[0]

    my_base = cls * slot_rows + rep * half_rows
    wanted = my_base.astype(f32) + row_i.astype(f32)

    def find(c, acc):
        t_c = targets_ref[c * n_rep + rep].astype(f32)
        return acc + jnp.where(t_c == wanted, (c + 1).astype(f32), 0.0)

    found = lax.fori_loop(0, n_cls, find, jnp.zeros((half_rows, half_rows), f32))
    src_col = jnp.sum(found, axis=1, keepdims=True) - 1.0
    src_row = to_row(src_col, eye)
    before = jnp.where((src_col == src_row) & (col_i < row_i), 1.0, 0.0)
    count_col = jnp.sum(before, axis=1, keepdims=True)
    seat_col = seat_of(src_col.astype(jnp.int32)) + count_col.astype(jnp.int32)
    seat_row = to_row(seat_col.astype(f32), eye).astype(jnp.int32)
    seat_i = lax.broadcasted_iota(jnp.int32, (half_rows, seats), 1)
    seating[...] = jnp.where(seat_i == seat_col, 1.0, 0.0).astype(bf16)
    turned_i = lax.broadcasted_iota(jnp.int32, (seats, half_rows), 0)
    turned = jnp.where(turned_i == seat_row, 1.0, 0.0).astype(bf16)
    loads[7].wait()
    free_seats[...] = jnp.dot(turned, free[...], preferred_element_type=f32)

    loads[5].wait()
    loads[6].wait()
    n_pos = positives_ref.shape[1]
    eye = eye_of(own_half)
    ids = []
    for p in range(n_pos):
        rows = [positives_ref[r, p : p + 1, :].astype(f32) for r in range(n_rep)]
        ids.append(jnp.concatenate([to_column(row, eye) for row in rows], axis=0).astype(jnp.int32))
    valid = jnp.zeros((n_query, 1), f32)
    for p in range(n_pos):
        valid = valid + jnp.where(ids[p] >= 0, 1.0, 0.0)
    id_counts[...] = jnp.broadcast_to(valid, id_counts.shape)
    slot_start = slot_ref[0] * slot_rows

    def counts_of(label):
        count = jnp.zeros((n_query, label.shape[1]), f32)
        for p in range(n_pos):
            count = count + jnp.where(ids[p] == label, 1.0, 0.0)
        return count

    fresh_base = cls * lab_rows + slot_start + rep * half_rows
    for part in range(PARTS):
        at_i = part * part_rows + lax.broadcasted_iota(jnp.int32, (half_rows, part_rows), 1)
        row_f = lax.broadcasted_iota(jnp.int32, (half_rows, part_rows), 0).astype(f32)
        at_row = jnp.sum(jnp.where(at_i == seat_col, row_f + 1.0, 0.0), axis=0, keepdims=True)
        fresh_seen[part] = at_row
        at_row = at_row.astype(jnp.int32)
        fresh_count[part] = counts_of(jnp.where(at_row > 0, fresh_base - 1 + at_row, -2))

    for k in range(chunks):
        loads[8 + k].wait()
        at = slice(k * slot_rows, (k + 1) * slot_rows)
        turned_labels[:, at] = labels[at].T
    query_copy(1, 0, n_cls - 1).wait_recv()
    side = q_slots.at[pl.ds(rep * n_cls, n_cls)]
    relay = pltpu.make_async_remote_copy(
        src_ref=side,
        dst_ref=side,
        send_sem=relay_sem.at[0],
        recv_sem=relay_sem.at[1],
        device_id=(cls, partner),
    )
    relay.start()
    relay.wait_recv()
    for s in range(n_cls * n_rep):
        q_rows[s * query_rows : (s + 1) * query_rows] = q_slots[s].astype(f32)
    q = q_rows[...].astype(bf16)

    def split(power):
        high = power.astype(bf16)
        return high, (power - high.astype(f32)).astype(bf16)

    def sums(block, power, count):
        exp_sum = jnp.sum(power, axis=1, keepdims=True)
        pos_sum = jnp.sum(count * jnp.where(count > 0.0, block, 0.0), axis=1, keepdims=True)
        return exp_sum, pos_sum

    n = n_query
    peak = jnp.full((n, 1), NEG, f32)
    for k in range(chunks):
        at = slice(k * slot_rows, (k + 1) * slot_rows)
        block = jnp.dot(q, turned_labels[:, at], preferred_element_type=f32)
        fresh = slot_start == rep * usable + k * slot_rows
        block = jnp.where(fresh, NEG, block)
        logits[:, at] = block
        peak = jnp.maximum(peak, jnp.max(block, axis=1, keepdims=True))
    grad = jnp.zeros((n, width), f32)
    hits = jnp.zeros((n, width), f32)
    exp_sum = jnp.zeros((n, 1), f32)
    pos_sum = jnp.zeros((n, 1), f32)
    for k in range(chunks):
        at = slice(k * slot_rows, (k + 1) * slot_rows)
        first = cls * lab_rows + rep * usable + k * slot_rows
        fresh = slot_start == rep * usable + k * slot_rows
        label = first + lax.broadcasted_iota(jnp.int32, (n, slot_rows), 1)
        count = jnp.where(fresh, 0.0, counts_of(label))
        block = logits[:, at]
        power = jnp.exp(block - peak)
        mixed[0:n], mixed[n : 2 * n] = split(power)
        mixed[2 * n : 3 * n] = count.astype(bf16)
        out = jnp.dot(mixed[...], labels[at], preferred_element_type=f32)
        e, s = sums(block, power, count)
        grad = grad + (out[0:n] + out[n : 2 * n])
        hits, exp_sum, pos_sum = hits + out[2 * n : 3 * n], exp_sum + e, pos_sum + s

    second = jnp.where(inner, 2, 1)
    for turn, part in enumerate((0, second, jnp.where(inner, 1, 3), jnp.where(inner, 3, 2))):
        low = part * span + (0 if turn else 1)
        row_copy(low, span if turn else span - 1, part).wait_recv()
        at = pl.ds(pl.multiple_of(part * part_rows, 16), part_rows)
        landed = [in_rows[part * span + k].astype(f32) for k in range(span)]
        vectors = (free_seats[at] + jnp.concatenate(landed, axis=0)).astype(bf16)
        fresh_rows[at] = vectors
        block = lax.dot_general(q, vectors, NT, preferred_element_type=f32)
        block = jnp.where(fresh_seen[part] > 0.0, block, NEG)
        top = jnp.maximum(peak, jnp.max(block, axis=1, keepdims=True))
        power = jnp.exp(block - top)
        high, rest = split(power)
        count = fresh_count[part]
        out = jnp.dot(
            jnp.concatenate([high, rest, count.astype(bf16)], axis=0), vectors, preferred_element_type=f32
        )
        e, s = sums(block, power, count)
        a = jnp.exp(peak - top)
        grad = grad * a + (out[0:n] + out[n : 2 * n])
        hits, exp_sum, pos_sum = hits + out[2 * n : 3 * n], exp_sum * a + e, pos_sum + s
        peak = top

    lane = lax.broadcasted_iota(jnp.int32, (n, STATS), 1)
    stats = jnp.where(lane == 0, peak, jnp.where(lane == 1, exp_sum, pos_sum))
    for r in range(n_rep):
        at = slice(r * own_half, (r + 1) * own_half)
        half_out[r, :, 0:width] = grad[at]
        half_out[r, :, width:] = stats[at]
        hits_out[r] = hits[at].astype(bf16)
    swaps = []
    for i, (a, b) in enumerate([(half_out, half_in), (hits_out, hits_in)]):
        swap = pltpu.make_async_remote_copy(
            src_ref=a.at[partner],
            dst_ref=b,
            send_sem=half_sem.at[i],
            recv_sem=half_sem.at[2 + i],
            device_id=(cls, partner),
        )
        swap.start()
        swaps.append(swap)
    x, xh = half_out[rep], hits_out[rep].astype(f32)
    some = id_counts[pl.ds(pl.multiple_of(rep * own_half, own_half), own_half), :][:, 0:1]
    for swap in swaps:
        swap.wait_recv()
    y, yh = half_in[...], hits_in[...].astype(f32)
    xs, ys = x[:, width:], y[:, width:]
    m = jnp.maximum(xs[:, 0:1], ys[:, 0:1])
    a, b = jnp.exp(xs[:, 0:1] - m), jnp.exp(ys[:, 0:1] - m)
    exp_sum = xs[:, 1:2] * a + ys[:, 1:2] * b
    pos_sum = xs[:, 2:3] + ys[:, 2:3]
    hits = xh + yh
    inv = 1.0 / exp_sum
    term = x[:, 0:width] * (a * inv) + y[:, 0:width] * (b * inv) - hits * (1.0 / some)
    lane = lax.broadcasted_iota(jnp.int32, (own_half, STATS), 1)
    stats = jnp.zeros((own_half, STATS), f32)
    for i, value in enumerate([m, exp_sum, pos_sum]):
        for j, piece in enumerate(thirds(value)):
            stats = jnp.where(lane == 3 * j + i, piece, stats)
    term, hits, stats = term.astype(bf16), hits.astype(bf16), stats.astype(bf16)
    for c in range(n_cls):
        at = slice(c * query_rows, (c + 1) * query_rows)
        shares_out[c, :, 0:width] = term[at]
        shares_out[c, :, width : 2 * width] = hits[at]
        shares_out[c, :, 2 * width :] = stats[at]

    def send_share(i):
        k = n_cls - 1 - i
        share_copy(k, cls ^ k, k, 1).start()

    each(n_cls - 1, send_share)
    shares_in[0] = shares_out[cls]

    refreshed = jnp.dot(seating[...], fresh_rows[...], preferred_element_type=f32)
    refreshed_ref[...] = refreshed.astype(bf16)
    pl.when(inner)(lambda: query_copy(1, 0, n_cls - 1).wait_send())
    row_copy(1, n_cls - 1, 0).wait_send()
    relay.wait_send()
    for swap in swaps:
        swap.wait_send()
    id_count = id_counts[pl.ds(mine * query_rows, query_rows), :][:, 0:1]

    share_copy(1, 0, 1, n_cls - 1).wait_recv()
    stats = shares_in[:, :, 2 * width :].astype(f32)
    stats = stats[:, :, 0:3] + stats[:, :, 3:6] + stats[:, :, 6:9]
    ms, es = stats[:, :, 0:1], stats[:, :, 1:2]
    pos_sum = jnp.sum(stats[:, :, 2:3], axis=0)
    m = jnp.max(ms, axis=0)
    es = es * jnp.exp(ms - m[None])
    exp_sum = jnp.sum(es, axis=0)
    rho = es * (1.0 / exp_sum)[None]
    inv = 1.0 / id_count
    back = (rho - 1.0) * inv[None]
    grad = jnp.zeros((query_rows, width), f32)
    for k in range(n_cls):
        grad = grad + rho[k] * shares_in[k, :, 0:width].astype(f32)
        grad = grad + back[k] * shares_in[k, :, width : 2 * width].astype(f32)
    loss = m + jnp.log(exp_sum) - pos_sum / id_count
    loss_ref[...] = to_row(loss, eye_of(query_rows))
    grads_ref[0] = grad.astype(bf16)
    share_copy(1, 0, 1, n_cls - 1).wait_send()


def pass_on(*refs):
    sem = refs[-1]
    half = len(refs) // 2
    copies = []
    for i, (source, target) in enumerate(zip(refs[:half], refs[half:-1])):
        copy = pltpu.make_async_copy(source, target, sem.at[i])
        copy.start()
        copies.append(copy)
    for copy in copies:
        copy.wait()


def per_device(
    n_cls,
    n_rep,
    queries,
    positives,
    label_vectors,
    refresh_slot,
    features,
    encoder_weight,
    encoder_gain,
    free_vectors,
    targets,
):
    f32, bf16 = jnp.float32, jnp.bfloat16
    total = n_cls * n_rep
    lab_rows, width = label_vectors.shape
    usable = lab_rows // n_rep
    slot_rows = lab_rows // SLOTS
    half_rows = slot_rows // n_rep
    per_owner = half_rows // n_cls
    padded = -(-per_owner // 8) * 8
    query_rows = queries.shape[1]
    n_query = total * query_rows
    own_half = n_query // n_rep
    n_pos = positives.shape[2]
    share = 2 * width + STATS
    vmem = pl.BlockSpec(memory_space=pltpu.VMEM)
    hbm = pl.BlockSpec(memory_space=pltpu.HBM)
    dma = pltpu.SemaphoreType.DMA
    outs = (
        ((1, query_rows), f32),
        ((1, query_rows, width), bf16),
        ((half_rows, width), bf16),
    )
    results = pl.pallas_call(
        functools.partial(step_kernel, n_cls, n_rep),
        out_shape=tuple(pltpu.VMEM(*out) for out in outs),
        in_specs=[hbm] * 9,
        out_specs=(vmem,) * 3,
        scratch_shapes=[
            pltpu.SMEM((1,), jnp.int32),
            pltpu.VMEM((n_rep, n_pos, own_half), jnp.int32),
            pltpu.VMEM((total, 1, half_rows), jnp.int32),
            pltpu.VMEM((width,), f32),
            pltpu.VMEM((usable, width), bf16),
            pltpu.VMEM((width, usable), bf16),
            pltpu.VMEM((half_rows, width), bf16),
            pltpu.VMEM((width, width), bf16),
            pltpu.VMEM((half_rows, width), bf16),
            pltpu.VMEM((n_cls * padded, width), f32),
            pltpu.VMEM((half_rows, n_cls * padded), bf16),
            pltpu.VMEM((n_cls * padded, width), bf16),
            pltpu.VMEM((PARTS, 1, n_cls // PARTS * padded), f32),
            pltpu.VMEM((PARTS, n_query, n_cls // PARTS * padded), f32),
            pltpu.VMEM((n_query, STATS), f32),
            pltpu.VMEM((total, query_rows, width), bf16),
            pltpu.VMEM((n_query, width), f32),
            pltpu.VMEM((n_cls, padded, width), bf16),
            pltpu.VMEM((n_cls, padded, width), bf16),
            pltpu.VMEM((n_query, usable), f32),
            pltpu.VMEM((3 * n_query, slot_rows), bf16),
            pltpu.VMEM((n_rep, own_half, width + STATS), f32),
            pltpu.VMEM((own_half, width + STATS), f32),
            pltpu.VMEM((n_rep, own_half, width), bf16),
            pltpu.VMEM((own_half, width), bf16),
            pltpu.VMEM((n_cls, query_rows, share), bf16),
            pltpu.VMEM((n_cls, query_rows, share), bf16),
            dma((8 + usable // slot_rows,)),
            dma((2,)),
            dma((2,)),
            dma,
            dma((PARTS,)),
            dma((4,)),
            dma((2,)),
        ],
        compiler_params=pltpu.CompilerParams(
            collective_id=0, has_side_effects=True, vmem_limit_bytes=48 * 2**20
        ),
    )(
        refresh_slot.reshape(1),
        *[
            pltpu.with_memory_space_constraint(x, pltpu.HBM)
            for x in (
                queries,
                positives.transpose(0, 2, 1),
                targets.reshape(total, 1, half_rows),
                encoder_gain,
                label_vectors,
                features,
                encoder_weight,
                free_vectors,
            )
        ]
    )
    return pl.pallas_call(
        pass_on,
        out_shape=tuple(jax.ShapeDtypeStruct(*out) for out in outs),
        in_specs=[vmem] * 3,
        out_specs=(hbm,) * 3,
        scratch_shapes=[dma((3,))],
    )(*[pltpu.with_memory_space_constraint(x, pltpu.VMEM) for x in results])


def solution(mesh):
    placed = (
        P("rep", "cls", None),
        P(),
        P("cls", None),
        P(),
        P(("cls", "rep"), None),
        P(),
        P(),
        P(("cls", "rep"), None),
        P(),
    )
    return jax.shard_map(
        functools.partial(per_device, mesh.shape["cls"], mesh.shape["rep"]),
        mesh=mesh,
        in_specs=placed,
        out_specs=(P("rep", "cls"), P("rep", "cls", None), P(("cls", "rep"), None)),
        check_vma=False,
    )
```

```python
import functools

import jax
import jax.numpy as jnp
from jax import lax
from jax.experimental import pallas as pl
from jax.experimental.pallas import tpu as pltpu
from jax.sharding import PartitionSpec as P

SLOTS = 8
NEG = -1e30
STATS = 128
PARTS = 4
PIECES = 8
NT = (((1,), (1,)), ((), ()))


def to_column(row, eye):
    return jnp.sum(jnp.where(eye, row, 0.0), axis=1, keepdims=True)


def to_row(col, eye):
    return jnp.sum(jnp.where(eye, col, 0.0), axis=0, keepdims=True)


def eye_of(n):
    shape = (n, n)
    return lax.broadcasted_iota(jnp.int32, shape, 0) == lax.broadcasted_iota(jnp.int32, shape, 1)


def each(count, step):
    if count <= 16:
        for i in range(count):
            step(i)
    else:
        lax.fori_loop(0, count, lambda i, carry: (step(i), carry)[1], 0)


def thirds(x):
    f32, bf16 = jnp.float32, jnp.bfloat16
    high = x.astype(bf16).astype(f32)
    rest = x - high
    mid = rest.astype(bf16).astype(f32)
    return high, mid, rest - mid


def step_kernel(
    n_cls,
    n_rep,
    slot_hbm,
    queries_hbm,
    positives_hbm,
    targets_hbm,
    gain_hbm,
    labels_hbm,
    features_hbm,
    weight_hbm,
    free_hbm,
    loss_ref,
    grads_ref,
    refreshed_ref,
    slot_ref,
    positives_ref,
    targets_ref,
    gain_ref,
    labels,
    turned_labels,
    features,
    weight,
    free,
    free_seats,
    seating,
    fresh_rows,
    fresh_seen,
    fresh_count,
    id_counts,
    q_slots,
    q_rows,
    out_rows,
    in_rows,
    logits,
    mixed,
    half_out,
    half_in,
    hits_out,
    hits_in,
    shares_out,
    shares_in,
    load_sem,
    q_sem,
    relay_sem,
    row_send,
    row_recv,
    half_sem,
    share_sem,
):
    f32, bf16 = jnp.float32, jnp.bfloat16
    cls = lax.axis_index("cls")
    rep = lax.axis_index("rep")
    partner = 1 - rep
    me = cls * n_rep + rep
    half_rows, width = features.shape
    padded = out_rows.shape[1]
    per_owner = half_rows // n_cls
    query_rows = q_slots.shape[1]
    n_query = q_rows.shape[0]
    own_half = n_query // n_rep
    usable, slot_rows = labels.shape[0], half_rows * n_rep
    lab_rows = usable * n_rep
    seats = n_cls * padded
    mine = rep * n_cls + cls
    span = n_cls // PARTS
    plane = cls // span
    inner = (plane > 0) & (plane < PARTS - 1)

    def seat_of(owner):
        return (owner ^ cls) * padded

    barrier = pltpu.get_barrier_semaphore()

    def greet(i):
        pl.semaphore_signal(barrier, inc=1, device_id=(cls ^ (n_cls - 1 - i), rep))

    each(n_cls - 1, greet)
    pl.semaphore_signal(barrier, inc=1, device_id=(cls, partner))

    chunks = usable // slot_rows
    pairs = [
        (features_hbm, features),
        (targets_hbm, targets_ref),
        (weight_hbm, weight),
        (gain_hbm, gain_ref),
        (queries_hbm.at[0], q_slots.at[mine]),
        (slot_hbm, slot_ref),
        (positives_hbm, positives_ref),
        (free_hbm, free),
    ]
    start = pl.multiple_of(rep * usable, slot_rows)
    pairs.append((labels_hbm.at[pl.ds(start, usable)], labels))
    loads = [pltpu.make_async_copy(a, b, load_sem.at[i]) for i, (a, b) in enumerate(pairs)]
    for copy in loads:
        copy.start()

    row_i = lax.broadcasted_iota(jnp.int32, (half_rows, half_rows), 0)
    col_i = lax.broadcasted_iota(jnp.int32, (half_rows, half_rows), 1)
    eye = row_i == col_i
    loads[1].wait()
    t_row = targets_ref[me].astype(f32)
    t_col = to_column(t_row, eye)
    rank = jnp.sum(jnp.where(t_col < t_row, 1.0, 0.0), axis=0, keepdims=True)
    owner = jnp.floor((rank + 0.5) * (1.0 / per_owner))
    seat_in = (rank - owner * per_owner).astype(jnp.int32)
    place = seat_of(owner.astype(jnp.int32)) + seat_in
    part_rows = span * padded

    def encode(low, high):
        rows = (high - low) * padded
        place_i = low * padded + lax.broadcasted_iota(jnp.int32, (rows, half_rows), 0)
        pick = jnp.where(place_i == place, 1.0, 0.0).astype(bf16)
        ordered = jnp.dot(pick, features[...], preferred_element_type=f32).astype(bf16)
        hidden = jnp.dot(ordered, weight[...], preferred_element_type=f32)
        scale = lax.rsqrt(jnp.mean(hidden * hidden, axis=1, keepdims=True) + 1e-06)
        encoded = hidden * scale * gain_ref[...].reshape(1, width)
        for k in range(low, high):
            out_rows[k] = encoded[(k - low) * padded : (k - low + 1) * padded].astype(bf16)

    loads[0].wait()
    loads[2].wait()
    loads[3].wait()
    encode(n_cls // 2, n_cls)
    loads[4].wait()

    pl.semaphore_wait(barrier, n_cls)

    def query_copy(k, slot, many):
        return pltpu.make_async_remote_copy(
            src_ref=q_slots.at[pl.ds(slot, many)],
            dst_ref=q_slots.at[pl.ds(slot, many)],
            send_sem=q_sem.at[0],
            recv_sem=q_sem.at[1],
            device_id=(cls ^ k, rep),
        )

    def row_copy(slot, many, part):
        return pltpu.make_async_remote_copy(
            src_ref=out_rows.at[pl.ds(slot, many)],
            dst_ref=in_rows.at[pl.ds(slot, many)],
            send_sem=row_send,
            recv_sem=row_recv.at[part],
            device_id=(cls ^ slot, rep),
        )

    def share_copy(k, source, slot, many):
        return pltpu.make_async_remote_copy(
            src_ref=shares_out.at[pl.ds(source, many)],
            dst_ref=shares_in.at[pl.ds(slot, many)],
            send_sem=share_sem.at[0],
            recv_sem=share_sem.at[1],
            device_id=(cls ^ k, rep),
        )

    def send_rows(part):
        top = (part + 1) * span - 1
        each(span if part else span - 1, lambda i: row_copy(top - i, 1, part).start())

    each(n_cls - 1, lambda i: query_copy(i + 1, mine, 1).start())
    pl.when(inner)(lambda: send_rows(2))
    encode(0, n_cls // 2)

    @pl.when(jnp.logical_not(inner))
    def _():
        query_copy(1, 0, n_cls - 1).wait_send()
        for part in (3, 2, 1, 0):
            send_rows(part)

    @pl.when(inner)
    def _():
        for part in (1, 0, 3):
            send_rows(part)

    in_rows[0] = out_rows[0]

    my_base = cls * slot_rows + rep * half_rows
    wanted = my_base.astype(f32) + row_i.astype(f32)

    def find(c, acc):
        t_c = targets_ref[c * n_rep + rep].astype(f32)
        return acc + jnp.where(t_c == wanted, (c + 1).astype(f32), 0.0)

    found = lax.fori_loop(0, n_cls, find, jnp.zeros((half_rows, half_rows), f32))
    src_col = jnp.sum(found, axis=1, keepdims=True) - 1.0
    src_row = to_row(src_col, eye)
    before = jnp.where((src_col == src_row) & (col_i < row_i), 1.0, 0.0)
    count_col = jnp.sum(before, axis=1, keepdims=True)
    seat_col = seat_of(src_col.astype(jnp.int32)) + count_col.astype(jnp.int32)
    seat_row = to_row(seat_col.astype(f32), eye).astype(jnp.int32)
    seat_i = lax.broadcasted_iota(jnp.int32, (half_rows, seats), 1)
    seating[...] = jnp.where(seat_i == seat_col, 1.0, 0.0).astype(bf16)
    turned_i = lax.broadcasted_iota(jnp.int32, (seats, half_rows), 0)
    turned = jnp.where(turned_i == seat_row, 1.0, 0.0).astype(bf16)
    loads[7].wait()
    free_seats[...] = jnp.dot(turned, free[...], preferred_element_type=f32)

    loads[5].wait()
    loads[6].wait()
    n_pos = positives_ref.shape[1]
    eye = eye_of(own_half)
    ids = []
    for p in range(n_pos):
        rows = [positives_ref[r, p : p + 1, :].astype(f32) for r in range(n_rep)]
        ids.append(jnp.concatenate([to_column(row, eye) for row in rows], axis=0).astype(jnp.int32))
    valid = jnp.zeros((n_query, 1), f32)
    for p in range(n_pos):
        valid = valid + jnp.where(ids[p] >= 0, 1.0, 0.0)
    id_counts[...] = jnp.broadcast_to(valid, id_counts.shape)
    slot_start = slot_ref[0] * slot_rows

    def counts_of(label):
        count = jnp.zeros((n_query, label.shape[1]), f32)
        for p in range(n_pos):
            count = count + jnp.where(ids[p] == label, 1.0, 0.0)
        return count

    fresh_base = cls * lab_rows + slot_start + rep * half_rows
    for part in range(PARTS):
        at_i = part * part_rows + lax.broadcasted_iota(jnp.int32, (half_rows, part_rows), 1)
        row_f = lax.broadcasted_iota(jnp.int32, (half_rows, part_rows), 0).astype(f32)
        at_row = jnp.sum(jnp.where(at_i == seat_col, row_f + 1.0, 0.0), axis=0, keepdims=True)
        fresh_seen[part] = at_row
        at_row = at_row.astype(jnp.int32)
        fresh_count[part] = counts_of(jnp.where(at_row > 0, fresh_base - 1 + at_row, -2))

    loads[8].wait()
    for k in range(chunks):
        at = slice(k * slot_rows, (k + 1) * slot_rows)
        turned_labels[:, at] = labels[at].T
    query_copy(1, 0, n_cls - 1).wait_recv()
    side = q_slots.at[pl.ds(rep * n_cls, n_cls)]
    relay = pltpu.make_async_remote_copy(
        src_ref=side,
        dst_ref=side,
        send_sem=relay_sem.at[0],
        recv_sem=relay_sem.at[1],
        device_id=(cls, partner),
    )
    relay.start()
    relay.wait_recv()
    for s in range(n_cls * n_rep):
        q_rows[s * query_rows : (s + 1) * query_rows] = q_slots[s].astype(f32)
    q = q_rows[...].astype(bf16)

    def split(power):
        high = power.astype(bf16)
        return high, (power - high.astype(f32)).astype(bf16)

    def sums(block, power, count):
        exp_sum = jnp.sum(power, axis=1, keepdims=True)
        pos_sum = jnp.sum(count * jnp.where(count > 0.0, block, 0.0), axis=1, keepdims=True)
        return exp_sum, pos_sum

    n = n_query
    peak = jnp.full((n, 1), NEG, f32)
    for k in range(chunks):
        at = slice(k * slot_rows, (k + 1) * slot_rows)
        block = jnp.dot(q, turned_labels[:, at], preferred_element_type=f32)
        fresh = slot_start == rep * usable + k * slot_rows
        block = jnp.where(fresh, NEG, block)
        logits[:, at] = block
        peak = jnp.maximum(peak, jnp.max(block, axis=1, keepdims=True))
    grad = jnp.zeros((n, width), f32)
    hits = jnp.zeros((n, width), f32)
    exp_sum = jnp.zeros((n, 1), f32)
    pos_sum = jnp.zeros((n, 1), f32)
    for k in range(chunks):
        at = slice(k * slot_rows, (k + 1) * slot_rows)
        first = cls * lab_rows + rep * usable + k * slot_rows
        fresh = slot_start == rep * usable + k * slot_rows
        label = first + lax.broadcasted_iota(jnp.int32, (n, slot_rows), 1)
        count = jnp.where(fresh, 0.0, counts_of(label))
        block = logits[:, at]
        power = jnp.exp(block - peak)
        mixed[0:n], mixed[n : 2 * n] = split(power)
        mixed[2 * n : 3 * n] = count.astype(bf16)
        out = jnp.dot(mixed[...], labels[at], preferred_element_type=f32)
        e, s = sums(block, power, count)
        grad = grad + (out[0:n] + out[n : 2 * n])
        hits, exp_sum, pos_sum = hits + out[2 * n : 3 * n], exp_sum + e, pos_sum + s

    second = jnp.where(inner, 2, 1)
    for turn, part in enumerate((0, second, jnp.where(inner, 1, 3), jnp.where(inner, 3, 2))):
        low = part * span + (0 if turn else 1)
        row_copy(low, span if turn else span - 1, part).wait_recv()
        at = pl.ds(pl.multiple_of(part * part_rows, 16), part_rows)
        landed = [in_rows[part * span + k].astype(f32) for k in range(span)]
        vectors = (free_seats[at] + jnp.concatenate(landed, axis=0)).astype(bf16)
        fresh_rows[at] = vectors
        block = lax.dot_general(q, vectors, NT, preferred_element_type=f32)
        block = jnp.where(fresh_seen[part] > 0.0, block, NEG)
        top = jnp.maximum(peak, jnp.max(block, axis=1, keepdims=True))
        power = jnp.exp(block - top)
        high, rest = split(power)
        count = fresh_count[part]
        out = jnp.dot(
            jnp.concatenate([high, rest, count.astype(bf16)], axis=0), vectors, preferred_element_type=f32
        )
        e, s = sums(block, power, count)
        a = jnp.exp(peak - top)
        grad = grad * a + (out[0:n] + out[n : 2 * n])
        hits, exp_sum, pos_sum = hits + out[2 * n : 3 * n], exp_sum * a + e, pos_sum + s
        peak = top

    lane = lax.broadcasted_iota(jnp.int32, (n, STATS), 1)
    stats = jnp.where(lane == 0, peak, jnp.where(lane == 1, exp_sum, pos_sum))
    for r in range(n_rep):
        at = slice(r * own_half, (r + 1) * own_half)
        half_out[r, :, 0:width] = grad[at]
        half_out[r, :, width:] = stats[at]
        hits_out[r] = hits[at].astype(bf16)
    swaps = []
    for i, (a, b) in enumerate([(half_out, half_in), (hits_out, hits_in)]):
        swap = pltpu.make_async_remote_copy(
            src_ref=a.at[partner],
            dst_ref=b,
            send_sem=half_sem.at[i],
            recv_sem=half_sem.at[2 + i],
            device_id=(cls, partner),
        )
        swap.start()
        swaps.append(swap)
    x, xh = half_out[rep], hits_out[rep].astype(f32)
    some = id_counts[pl.ds(pl.multiple_of(rep * own_half, own_half), own_half), :][:, 0:1]
    for swap in swaps:
        swap.wait_recv()
    y, yh = half_in[...], hits_in[...].astype(f32)
    xs, ys = x[:, width:], y[:, width:]
    m = jnp.maximum(xs[:, 0:1], ys[:, 0:1])
    a, b = jnp.exp(xs[:, 0:1] - m), jnp.exp(ys[:, 0:1] - m)
    exp_sum = xs[:, 1:2] * a + ys[:, 1:2] * b
    pos_sum = xs[:, 2:3] + ys[:, 2:3]
    hits = xh + yh
    inv = 1.0 / exp_sum
    term = x[:, 0:width] * (a * inv) + y[:, 0:width] * (b * inv) - hits * (1.0 / some)
    lane = lax.broadcasted_iota(jnp.int32, (own_half, STATS), 1)
    stats = jnp.zeros((own_half, STATS), f32)
    for i, value in enumerate([m, exp_sum, pos_sum]):
        for j, piece in enumerate(thirds(value)):
            stats = jnp.where(lane == 3 * j + i, piece, stats)
    term, hits, stats = term.astype(bf16), hits.astype(bf16), stats.astype(bf16)
    for c in range(n_cls):
        at = slice(c * query_rows, (c + 1) * query_rows)
        shares_out[c, :, 0:width] = term[at]
        shares_out[c, :, width : 2 * width] = hits[at]
        shares_out[c, :, 2 * width :] = stats[at]

    def send_share(i):
        other = i + (cls <= i).astype(jnp.int32)
        share_copy(cls ^ other, other, cls ^ other, 1).start()

    each(n_cls - 1, send_share)
    shares_in[0] = shares_out[cls]

    refreshed = jnp.dot(seating[...], fresh_rows[...], preferred_element_type=f32)
    refreshed_ref[...] = refreshed.astype(bf16)
    pl.when(inner)(lambda: query_copy(1, 0, n_cls - 1).wait_send())
    row_copy(1, n_cls - 1, 0).wait_send()
    relay.wait_send()
    for swap in swaps:
        swap.wait_send()
    id_count = id_counts[pl.ds(mine * query_rows, query_rows), :][:, 0:1]

    share_copy(1, 0, 1, n_cls - 1).wait_recv()
    stats = shares_in[:, :, 2 * width :].astype(f32)
    stats = stats[:, :, 0:3] + stats[:, :, 3:6] + stats[:, :, 6:9]
    ms, es = stats[:, :, 0:1], stats[:, :, 1:2]
    pos_sum = jnp.sum(stats[:, :, 2:3], axis=0)
    m = jnp.max(ms, axis=0)
    es = es * jnp.exp(ms - m[None])
    exp_sum = jnp.sum(es, axis=0)
    rho = es * (1.0 / exp_sum)[None]
    inv = 1.0 / id_count
    back = (rho - 1.0) * inv[None]
    grad = jnp.zeros((query_rows, width), f32)
    for k in range(n_cls):
        grad = grad + rho[k] * shares_in[k, :, 0:width].astype(f32)
        grad = grad + back[k] * shares_in[k, :, width : 2 * width].astype(f32)
    loss = m + jnp.log(exp_sum) - pos_sum / id_count
    loss_ref[...] = to_row(loss, eye_of(query_rows))
    grads_ref[0] = grad.astype(bf16)
    share_copy(1, 0, 1, n_cls - 1).wait_send()


def pass_on(loss, grads, refreshed, loss_hbm, grads_hbm, refreshed_hbm, sem):
    rows = refreshed.shape[0] // PIECES
    for i in range(PIECES):
        at = pl.ds(i * rows, rows)
        pltpu.make_async_copy(refreshed.at[at], refreshed_hbm.at[at], sem.at[2]).start()
    small = [
        pltpu.make_async_copy(loss, loss_hbm, sem.at[0]),
        pltpu.make_async_copy(grads, grads_hbm, sem.at[1]),
    ]
    for copy in small:
        copy.start()
    for copy in small:
        copy.wait()
    pltpu.make_async_copy(refreshed, refreshed_hbm, sem.at[2]).wait()


def per_device(
    n_cls,
    n_rep,
    queries,
    positives,
    label_vectors,
    refresh_slot,
    features,
    encoder_weight,
    encoder_gain,
    free_vectors,
    targets,
):
    f32, bf16 = jnp.float32, jnp.bfloat16
    total = n_cls * n_rep
    lab_rows, width = label_vectors.shape
    usable = lab_rows // n_rep
    slot_rows = lab_rows // SLOTS
    half_rows = slot_rows // n_rep
    per_owner = half_rows // n_cls
    padded = -(-per_owner // 8) * 8
    query_rows = queries.shape[1]
    n_query = total * query_rows
    own_half = n_query // n_rep
    n_pos = positives.shape[2]
    share = 2 * width + STATS
    vmem = pl.BlockSpec(memory_space=pltpu.VMEM)
    hbm = pl.BlockSpec(memory_space=pltpu.HBM)
    dma = pltpu.SemaphoreType.DMA
    outs = (
        ((1, query_rows), f32),
        ((1, query_rows, width), bf16),
        ((half_rows, width), bf16),
    )
    results = pl.pallas_call(
        functools.partial(step_kernel, n_cls, n_rep),
        out_shape=tuple(pltpu.VMEM(*out) for out in outs),
        in_specs=[hbm] * 9,
        out_specs=(vmem,) * 3,
        scratch_shapes=[
            pltpu.SMEM((1,), jnp.int32),
            pltpu.VMEM((n_rep, n_pos, own_half), jnp.int32),
            pltpu.VMEM((total, 1, half_rows), jnp.int32),
            pltpu.VMEM((width,), f32),
            pltpu.VMEM((usable, width), bf16),
            pltpu.VMEM((width, usable), bf16),
            pltpu.VMEM((half_rows, width), bf16),
            pltpu.VMEM((width, width), bf16),
            pltpu.VMEM((half_rows, width), bf16),
            pltpu.VMEM((n_cls * padded, width), f32),
            pltpu.VMEM((half_rows, n_cls * padded), bf16),
            pltpu.VMEM((n_cls * padded, width), bf16),
            pltpu.VMEM((PARTS, 1, n_cls // PARTS * padded), f32),
            pltpu.VMEM((PARTS, n_query, n_cls // PARTS * padded), f32),
            pltpu.VMEM((n_query, STATS), f32),
            pltpu.VMEM((total, query_rows, width), bf16),
            pltpu.VMEM((n_query, width), f32),
            pltpu.VMEM((n_cls, padded, width), bf16),
            pltpu.VMEM((n_cls, padded, width), bf16),
            pltpu.VMEM((n_query, usable), f32),
            pltpu.VMEM((3 * n_query, slot_rows), bf16),
            pltpu.VMEM((n_rep, own_half, width + STATS), f32),
            pltpu.VMEM((own_half, width + STATS), f32),
            pltpu.VMEM((n_rep, own_half, width), bf16),
            pltpu.VMEM((own_half, width), bf16),
            pltpu.VMEM((n_cls, query_rows, share), bf16),
            pltpu.VMEM((n_cls, query_rows, share), bf16),
            dma((9,)),
            dma((2,)),
            dma((2,)),
            dma,
            dma((PARTS,)),
            dma((4,)),
            dma((2,)),
        ],
        compiler_params=pltpu.CompilerParams(
            collective_id=0, has_side_effects=True, vmem_limit_bytes=48 * 2**20
        ),
    )(
        refresh_slot.reshape(1),
        *[
            pltpu.with_memory_space_constraint(x, pltpu.HBM)
            for x in (
                queries,
                positives.transpose(0, 2, 1),
                targets.reshape(total, 1, half_rows),
                encoder_gain,
                label_vectors,
                features,
                encoder_weight,
                free_vectors,
            )
        ]
    )
    return pl.pallas_call(
        pass_on,
        out_shape=tuple(jax.ShapeDtypeStruct(*out) for out in outs),
        in_specs=[vmem] * 3,
        out_specs=(hbm,) * 3,
        scratch_shapes=[dma((3,))],
    )(*[pltpu.with_memory_space_constraint(x, pltpu.VMEM) for x in results])


def solution(mesh):
    placed = (
        P("rep", "cls", None),
        P(),
        P("cls", None),
        P(),
        P(("cls", "rep"), None),
        P(),
        P(),
        P(("cls", "rep"), None),
        P(),
    )
    return jax.shard_map(
        functools.partial(per_device, mesh.shape["cls"], mesh.shape["rep"]),
        mesh=mesh,
        in_specs=placed,
        out_specs=(P("rep", "cls"), P("rep", "cls", None), P(("cls", "rep"), None)),
        check_vma=False,
    )
```

```python
import functools

import jax
import jax.numpy as jnp
from jax import lax
from jax.experimental import pallas as pl
from jax.experimental.pallas import tpu as pltpu
from jax.sharding import PartitionSpec as P

SLOTS = 8
NEG = -1e30
STATS = 128
PARTS = 4
PIECES = 8
NT = (((1,), (1,)), ((), ()))


def to_column(row, eye):
    return jnp.sum(jnp.where(eye, row, 0.0), axis=1, keepdims=True)


def to_row(col, eye):
    return jnp.sum(jnp.where(eye, col, 0.0), axis=0, keepdims=True)


def eye_of(n):
    shape = (n, n)
    return lax.broadcasted_iota(jnp.int32, shape, 0) == lax.broadcasted_iota(jnp.int32, shape, 1)


def each(count, step):
    if count <= 16:
        for i in range(count):
            step(i)
    else:
        lax.fori_loop(0, count, lambda i, carry: (step(i), carry)[1], 0)


def thirds(x):
    f32, bf16 = jnp.float32, jnp.bfloat16
    high = x.astype(bf16).astype(f32)
    rest = x - high
    mid = rest.astype(bf16).astype(f32)
    return high, mid, rest - mid


def step_kernel(
    n_cls,
    n_rep,
    slot_hbm,
    queries_hbm,
    positives_hbm,
    targets_hbm,
    gain_hbm,
    labels_hbm,
    features_hbm,
    weight_hbm,
    free_hbm,
    loss_ref,
    grads_ref,
    refreshed_ref,
    slot_ref,
    positives_ref,
    targets_ref,
    gain_ref,
    labels,
    turned_labels,
    features,
    weight,
    free,
    free_seats,
    seating,
    fresh_rows,
    fresh_seen,
    fresh_count,
    id_counts,
    q_slots,
    q_rows,
    out_rows,
    in_rows,
    logits,
    mixed,
    half_out,
    half_in,
    hits_out,
    hits_in,
    shares_out,
    shares_in,
    load_sem,
    q_sem,
    relay_sem,
    row_send,
    row_recv,
    half_sem,
    share_sem,
):
    f32, bf16 = jnp.float32, jnp.bfloat16
    cls = lax.axis_index("cls")
    rep = lax.axis_index("rep")
    partner = 1 - rep
    me = cls * n_rep + rep
    half_rows, width = features.shape
    padded = out_rows.shape[1]
    per_owner = half_rows // n_cls
    query_rows = q_slots.shape[1]
    n_query = q_rows.shape[0]
    own_half = n_query // n_rep
    usable, slot_rows = labels.shape[0], half_rows * n_rep
    lab_rows = usable * n_rep
    seats = n_cls * padded
    mine = rep * n_cls + cls
    span = n_cls // PARTS
    plane = cls // span
    inner = (plane > 0) & (plane < PARTS - 1)

    def seat_of(owner):
        return (owner ^ cls) * padded

    barrier = pltpu.get_barrier_semaphore()

    def greet(i):
        pl.semaphore_signal(barrier, inc=1, device_id=(cls ^ (n_cls - 1 - i), rep))

    each(n_cls - 1, greet)
    pl.semaphore_signal(barrier, inc=1, device_id=(cls, partner))

    chunks = usable // slot_rows
    pairs = [
        (features_hbm, features),
        (targets_hbm, targets_ref),
        (weight_hbm, weight),
        (gain_hbm, gain_ref),
        (queries_hbm.at[0], q_slots.at[mine]),
        (slot_hbm, slot_ref),
        (positives_hbm, positives_ref),
        (free_hbm, free),
    ]
    start = pl.multiple_of(rep * usable, slot_rows)
    pairs.append((labels_hbm.at[pl.ds(start, usable)], labels))
    loads = [pltpu.make_async_copy(a, b, load_sem.at[i]) for i, (a, b) in enumerate(pairs)]
    for copy in loads:
        copy.start()

    row_i = lax.broadcasted_iota(jnp.int32, (half_rows, half_rows), 0)
    col_i = lax.broadcasted_iota(jnp.int32, (half_rows, half_rows), 1)
    eye = row_i == col_i
    loads[1].wait()
    t_row = targets_ref[me].astype(f32)
    t_col = to_column(t_row, eye)
    rank = jnp.sum(jnp.where(t_col < t_row, 1.0, 0.0), axis=0, keepdims=True)
    owner = jnp.floor((rank + 0.5) * (1.0 / per_owner))
    seat_in = (rank - owner * per_owner).astype(jnp.int32)
    place = seat_of(owner.astype(jnp.int32)) + seat_in
    part_rows = span * padded

    def encode(low, high):
        rows = (high - low) * padded
        place_i = low * padded + lax.broadcasted_iota(jnp.int32, (rows, half_rows), 0)
        pick = jnp.where(place_i == place, 1.0, 0.0).astype(bf16)
        ordered = jnp.dot(pick, features[...], preferred_element_type=f32).astype(bf16)
        hidden = jnp.dot(ordered, weight[...], preferred_element_type=f32)
        scale = lax.rsqrt(jnp.mean(hidden * hidden, axis=1, keepdims=True) + 1e-06)
        encoded = hidden * scale * gain_ref[...].reshape(1, width)
        for k in range(low, high):
            out_rows[k] = encoded[(k - low) * padded : (k - low + 1) * padded].astype(bf16)

    loads[0].wait()
    loads[2].wait()
    loads[3].wait()
    encode(n_cls // 2, n_cls)
    loads[4].wait()

    pl.semaphore_wait(barrier, n_cls)

    def query_copy(k, slot, many):
        return pltpu.make_async_remote_copy(
            src_ref=q_slots.at[pl.ds(slot, many)],
            dst_ref=q_slots.at[pl.ds(slot, many)],
            send_sem=q_sem.at[0],
            recv_sem=q_sem.at[1],
            device_id=(cls ^ k, rep),
        )

    def row_copy(slot, many, part):
        return pltpu.make_async_remote_copy(
            src_ref=out_rows.at[pl.ds(slot, many)],
            dst_ref=in_rows.at[pl.ds(slot, many)],
            send_sem=row_send,
            recv_sem=row_recv.at[part],
            device_id=(cls ^ slot, rep),
        )

    def share_copy(k, source, slot, many):
        return pltpu.make_async_remote_copy(
            src_ref=shares_out.at[pl.ds(source, many)],
            dst_ref=shares_in.at[pl.ds(slot, many)],
            send_sem=share_sem.at[0],
            recv_sem=share_sem.at[1],
            device_id=(cls ^ k, rep),
        )

    def send_rows(part):
        top = (part + 1) * span - 1
        each(span if part else span - 1, lambda i: row_copy(top - i, 1, part).start())

    each(n_cls - 1, lambda i: query_copy(i + 1, mine, 1).start())
    pl.when(inner)(lambda: send_rows(2))
    encode(0, n_cls // 2)

    @pl.when(jnp.logical_not(inner))
    def _():
        query_copy(1, 0, n_cls - 1).wait_send()
        for part in (3, 2, 1, 0):
            send_rows(part)

    @pl.when(inner)
    def _():
        for part in (1, 0, 3):
            send_rows(part)

    in_rows[0] = out_rows[0]

    my_base = cls * slot_rows + rep * half_rows
    wanted = my_base.astype(f32) + row_i.astype(f32)

    def find(c, acc):
        t_c = targets_ref[c * n_rep + rep].astype(f32)
        return acc + jnp.where(t_c == wanted, (c + 1).astype(f32), 0.0)

    found = lax.fori_loop(0, n_cls, find, jnp.zeros((half_rows, half_rows), f32))
    src_col = jnp.sum(found, axis=1, keepdims=True) - 1.0
    src_row = to_row(src_col, eye)
    before = jnp.where((src_col == src_row) & (col_i < row_i), 1.0, 0.0)
    count_col = jnp.sum(before, axis=1, keepdims=True)
    seat_col = seat_of(src_col.astype(jnp.int32)) + count_col.astype(jnp.int32)
    seat_row = to_row(seat_col.astype(f32), eye).astype(jnp.int32)
    seat_i = lax.broadcasted_iota(jnp.int32, (half_rows, seats), 1)
    seating[...] = jnp.where(seat_i == seat_col, 1.0, 0.0).astype(bf16)
    turned_i = lax.broadcasted_iota(jnp.int32, (seats, half_rows), 0)
    turned = jnp.where(turned_i == seat_row, 1.0, 0.0).astype(bf16)
    loads[7].wait()
    free_seats[...] = jnp.dot(turned, free[...], preferred_element_type=f32)

    loads[5].wait()
    loads[6].wait()
    n_pos = positives_ref.shape[1]
    eye = eye_of(own_half)
    ids = []
    for p in range(n_pos):
        rows = [positives_ref[r, p : p + 1, :].astype(f32) for r in range(n_rep)]
        ids.append(jnp.concatenate([to_column(row, eye) for row in rows], axis=0).astype(jnp.int32))
    valid = jnp.zeros((n_query, 1), f32)
    for p in range(n_pos):
        valid = valid + jnp.where(ids[p] >= 0, 1.0, 0.0)
    id_counts[...] = jnp.broadcast_to(valid, id_counts.shape)
    slot_start = slot_ref[0] * slot_rows

    def counts_of(label):
        count = jnp.zeros((n_query, label.shape[1]), f32)
        for p in range(n_pos):
            count = count + jnp.where(ids[p] == label, 1.0, 0.0)
        return count

    fresh_base = cls * lab_rows + slot_start + rep * half_rows
    for part in range(PARTS):
        at_i = part * part_rows + lax.broadcasted_iota(jnp.int32, (half_rows, part_rows), 1)
        row_f = lax.broadcasted_iota(jnp.int32, (half_rows, part_rows), 0).astype(f32)
        at_row = jnp.sum(jnp.where(at_i == seat_col, row_f + 1.0, 0.0), axis=0, keepdims=True)
        fresh_seen[part] = at_row
        at_row = at_row.astype(jnp.int32)
        fresh_count[part] = counts_of(jnp.where(at_row > 0, fresh_base - 1 + at_row, -2))

    loads[8].wait()
    for k in range(chunks):
        at = slice(k * slot_rows, (k + 1) * slot_rows)
        turned_labels[:, at] = labels[at].T
    query_copy(1, 0, n_cls - 1).wait_recv()
    side = q_slots.at[pl.ds(rep * n_cls, n_cls)]
    relay = pltpu.make_async_remote_copy(
        src_ref=side,
        dst_ref=side,
        send_sem=relay_sem.at[0],
        recv_sem=relay_sem.at[1],
        device_id=(cls, partner),
    )
    relay.start()
    relay.wait_recv()
    for s in range(n_cls * n_rep):
        q_rows[s * query_rows : (s + 1) * query_rows] = q_slots[s].astype(f32)
    q = q_rows[...].astype(bf16)

    def split(power):
        high = power.astype(bf16)
        return high, (power - high.astype(f32)).astype(bf16)

    def sums(block, power, count):
        exp_sum = jnp.sum(power, axis=1, keepdims=True)
        pos_sum = jnp.sum(count * jnp.where(count > 0.0, block, 0.0), axis=1, keepdims=True)
        return exp_sum, pos_sum

    n = n_query
    peak = jnp.full((n, 1), NEG, f32)
    for k in range(chunks):
        at = slice(k * slot_rows, (k + 1) * slot_rows)
        block = jnp.dot(q, turned_labels[:, at], preferred_element_type=f32)
        fresh = slot_start == rep * usable + k * slot_rows
        block = jnp.where(fresh, NEG, block)
        logits[:, at] = block
        peak = jnp.maximum(peak, jnp.max(block, axis=1, keepdims=True))
    grad = jnp.zeros((n, width), f32)
    hits = jnp.zeros((n, width), f32)
    exp_sum = jnp.zeros((n, 1), f32)
    pos_sum = jnp.zeros((n, 1), f32)
    for k in range(chunks):
        at = slice(k * slot_rows, (k + 1) * slot_rows)
        first = cls * lab_rows + rep * usable + k * slot_rows
        fresh = slot_start == rep * usable + k * slot_rows
        label = first + lax.broadcasted_iota(jnp.int32, (n, slot_rows), 1)
        count = jnp.where(fresh, 0.0, counts_of(label))
        block = logits[:, at]
        power = jnp.exp(block - peak)
        mixed[0:n], mixed[n : 2 * n] = split(power)
        mixed[2 * n : 3 * n] = count.astype(bf16)
        out = jnp.dot(mixed[...], labels[at], preferred_element_type=f32)
        e, s = sums(block, power, count)
        grad = grad + (out[0:n] + out[n : 2 * n])
        hits, exp_sum, pos_sum = hits + out[2 * n : 3 * n], exp_sum + e, pos_sum + s

    second = jnp.where(inner, 2, 1)
    for turn, part in enumerate((0, second, jnp.where(inner, 1, 3), jnp.where(inner, 3, 2))):
        low = part * span + (0 if turn else 1)
        row_copy(low, span if turn else span - 1, part).wait_recv()
        at = pl.ds(pl.multiple_of(part * part_rows, 16), part_rows)
        landed = [in_rows[part * span + k].astype(f32) for k in range(span)]
        vectors = (free_seats[at] + jnp.concatenate(landed, axis=0)).astype(bf16)
        fresh_rows[at] = vectors
        block = lax.dot_general(q, vectors, NT, preferred_element_type=f32)
        block = jnp.where(fresh_seen[part] > 0.0, block, NEG)
        top = jnp.maximum(peak, jnp.max(block, axis=1, keepdims=True))
        power = jnp.exp(block - top)
        high, rest = split(power)
        count = fresh_count[part]
        out = jnp.dot(
            jnp.concatenate([high, rest, count.astype(bf16)], axis=0), vectors, preferred_element_type=f32
        )
        e, s = sums(block, power, count)
        a = jnp.exp(peak - top)
        grad = grad * a + (out[0:n] + out[n : 2 * n])
        hits, exp_sum, pos_sum = hits + out[2 * n : 3 * n], exp_sum * a + e, pos_sum + s
        peak = top

    lane = lax.broadcasted_iota(jnp.int32, (n, STATS), 1)
    stats = jnp.where(lane == 0, peak, jnp.where(lane == 1, exp_sum, pos_sum))
    for r in range(n_rep):
        at = slice(r * own_half, (r + 1) * own_half)
        half_out[r, :, 0:width] = grad[at]
        half_out[r, :, width:] = stats[at]
        hits_out[r] = hits[at].astype(bf16)
    swaps = []
    for i, (a, b) in enumerate([(half_out, half_in), (hits_out, hits_in)]):
        swap = pltpu.make_async_remote_copy(
            src_ref=a.at[partner],
            dst_ref=b,
            send_sem=half_sem.at[i],
            recv_sem=half_sem.at[2 + i],
            device_id=(cls, partner),
        )
        swap.start()
        swaps.append(swap)
    x, xh = half_out[rep], hits_out[rep].astype(f32)
    some = id_counts[pl.ds(pl.multiple_of(rep * own_half, own_half), own_half), :]
    for swap in swaps:
        swap.wait_recv()
    y, yh = half_in[...], hits_in[...].astype(f32)
    tiles = width // STATS

    def wide(v):
        return jnp.concatenate([v] * tiles, axis=1)

    def spread(v, i):
        return jnp.broadcast_to(v[:, width + i : width + i + 1], some.shape)

    xm, ym = spread(x, 0), spread(y, 0)
    m = jnp.maximum(xm, ym)
    a, b = jnp.exp(xm - m), jnp.exp(ym - m)
    exp_sum = spread(x, 1) * a + spread(y, 1) * b
    pos_sum = spread(x, 2) + spread(y, 2)
    hits = xh + yh
    inv = 1.0 / exp_sum
    term = x[:, 0:width] * wide(a * inv) + y[:, 0:width] * wide(b * inv) - hits * wide(1.0 / some)
    lane = lax.broadcasted_iota(jnp.int32, (own_half, STATS), 1)
    stats = jnp.zeros((own_half, STATS), f32)
    for i, value in enumerate([m, exp_sum, pos_sum]):
        for j, piece in enumerate(thirds(value)):
            stats = jnp.where(lane == 3 * j + i, piece, stats)
    term, hits, stats = term.astype(bf16), hits.astype(bf16), stats.astype(bf16)
    for c in range(n_cls):
        at = slice(c * query_rows, (c + 1) * query_rows)
        shares_out[c, :, 0:width] = term[at]
        shares_out[c, :, width : 2 * width] = hits[at]
        shares_out[c, :, 2 * width :] = stats[at]

    def send_share(i):
        other = i + (cls <= i).astype(jnp.int32)
        share_copy(cls ^ other, other, cls ^ other, 1).start()

    each(n_cls - 1, send_share)
    shares_in[0] = shares_out[cls]

    refreshed = jnp.dot(seating[...], fresh_rows[...], preferred_element_type=f32)
    refreshed_ref[...] = refreshed.astype(bf16)
    pl.when(inner)(lambda: query_copy(1, 0, n_cls - 1).wait_send())
    row_copy(1, n_cls - 1, 0).wait_send()
    relay.wait_send()
    for swap in swaps:
        swap.wait_send()
    id_count = id_counts[pl.ds(mine * query_rows, query_rows), :][:, 0:1]

    share_copy(1, 0, 1, n_cls - 1).wait_recv()
    stats = jnp.concatenate([shares_in[k, :, 2 * width :].astype(f32) for k in range(n_cls)], axis=0)

    def gather(i):
        parts = [jnp.broadcast_to(stats[:, 3 * j + i : 3 * j + i + 1], stats.shape) for j in range(3)]
        whole = parts[0] + parts[1] + parts[2]
        return [whole[k * query_rows : (k + 1) * query_rows] for k in range(n_cls)]

    ms, es, ps = gather(0), gather(1), gather(2)
    m = functools.reduce(jnp.maximum, ms)
    es = [e * jnp.exp(x - m) for e, x in zip(es, ms)]
    exp_sum = functools.reduce(jnp.add, es)
    pos_sum = functools.reduce(jnp.add, ps)
    inv, inv_count = 1.0 / exp_sum, 1.0 / id_count
    grad = jnp.zeros((query_rows, width), f32)
    for k in range(n_cls):
        rho = es[k] * inv
        back = (rho - 1.0) * inv_count
        grad = grad + wide(rho) * shares_in[k, :, 0:width].astype(f32)
        grad = grad + wide(back) * shares_in[k, :, width : 2 * width].astype(f32)
    loss = (m + jnp.log(exp_sum))[:, 0:1] - pos_sum[:, 0:1] * inv_count
    loss_ref[...] = to_row(loss, eye_of(query_rows))
    grads_ref[0] = grad.astype(bf16)
    share_copy(1, 0, 1, n_cls - 1).wait_send()


def pass_on(loss, grads, refreshed, loss_hbm, grads_hbm, refreshed_hbm, sem):
    rows = refreshed.shape[0] // PIECES
    for i in range(PIECES):
        at = pl.ds(i * rows, rows)
        pltpu.make_async_copy(refreshed.at[at], refreshed_hbm.at[at], sem.at[2]).start()
    small = [
        pltpu.make_async_copy(loss, loss_hbm, sem.at[0]),
        pltpu.make_async_copy(grads, grads_hbm, sem.at[1]),
    ]
    for copy in small:
        copy.start()
    for copy in small:
        copy.wait()
    pltpu.make_async_copy(refreshed, refreshed_hbm, sem.at[2]).wait()


def per_device(
    n_cls,
    n_rep,
    queries,
    positives,
    label_vectors,
    refresh_slot,
    features,
    encoder_weight,
    encoder_gain,
    free_vectors,
    targets,
):
    f32, bf16 = jnp.float32, jnp.bfloat16
    total = n_cls * n_rep
    lab_rows, width = label_vectors.shape
    usable = lab_rows // n_rep
    slot_rows = lab_rows // SLOTS
    half_rows = slot_rows // n_rep
    per_owner = half_rows // n_cls
    padded = -(-per_owner // 8) * 8
    query_rows = queries.shape[1]
    n_query = total * query_rows
    own_half = n_query // n_rep
    n_pos = positives.shape[2]
    share = 2 * width + STATS
    vmem = pl.BlockSpec(memory_space=pltpu.VMEM)
    hbm = pl.BlockSpec(memory_space=pltpu.HBM)
    dma = pltpu.SemaphoreType.DMA
    outs = (
        ((1, query_rows), f32),
        ((1, query_rows, width), bf16),
        ((half_rows, width), bf16),
    )
    results = pl.pallas_call(
        functools.partial(step_kernel, n_cls, n_rep),
        out_shape=tuple(pltpu.VMEM(*out) for out in outs),
        in_specs=[hbm] * 9,
        out_specs=(vmem,) * 3,
        scratch_shapes=[
            pltpu.SMEM((1,), jnp.int32),
            pltpu.VMEM((n_rep, n_pos, own_half), jnp.int32),
            pltpu.VMEM((total, 1, half_rows), jnp.int32),
            pltpu.VMEM((width,), f32),
            pltpu.VMEM((usable, width), bf16),
            pltpu.VMEM((width, usable), bf16),
            pltpu.VMEM((half_rows, width), bf16),
            pltpu.VMEM((width, width), bf16),
            pltpu.VMEM((half_rows, width), bf16),
            pltpu.VMEM((n_cls * padded, width), f32),
            pltpu.VMEM((half_rows, n_cls * padded), bf16),
            pltpu.VMEM((n_cls * padded, width), bf16),
            pltpu.VMEM((PARTS, 1, n_cls // PARTS * padded), f32),
            pltpu.VMEM((PARTS, n_query, n_cls // PARTS * padded), f32),
            pltpu.VMEM((n_query, STATS), f32),
            pltpu.VMEM((total, query_rows, width), bf16),
            pltpu.VMEM((n_query, width), f32),
            pltpu.VMEM((n_cls, padded, width), bf16),
            pltpu.VMEM((n_cls, padded, width), bf16),
            pltpu.VMEM((n_query, usable), f32),
            pltpu.VMEM((3 * n_query, slot_rows), bf16),
            pltpu.VMEM((n_rep, own_half, width + STATS), f32),
            pltpu.VMEM((own_half, width + STATS), f32),
            pltpu.VMEM((n_rep, own_half, width), bf16),
            pltpu.VMEM((own_half, width), bf16),
            pltpu.VMEM((n_cls, query_rows, share), bf16),
            pltpu.VMEM((n_cls, query_rows, share), bf16),
            dma((9,)),
            dma((2,)),
            dma((2,)),
            dma,
            dma((PARTS,)),
            dma((4,)),
            dma((2,)),
        ],
        compiler_params=pltpu.CompilerParams(
            collective_id=0, has_side_effects=True, vmem_limit_bytes=48 * 2**20
        ),
    )(
        refresh_slot.reshape(1),
        *[
            pltpu.with_memory_space_constraint(x, pltpu.HBM)
            for x in (
                queries,
                positives.transpose(0, 2, 1),
                targets.reshape(total, 1, half_rows),
                encoder_gain,
                label_vectors,
                features,
                encoder_weight,
                free_vectors,
            )
        ]
    )
    return pl.pallas_call(
        pass_on,
        out_shape=tuple(jax.ShapeDtypeStruct(*out) for out in outs),
        in_specs=[vmem] * 3,
        out_specs=(hbm,) * 3,
        scratch_shapes=[dma((3,))],
    )(*[pltpu.with_memory_space_constraint(x, pltpu.VMEM) for x in results])


def solution(mesh):
    placed = (
        P("rep", "cls", None),
        P(),
        P("cls", None),
        P(),
        P(("cls", "rep"), None),
        P(),
        P(),
        P(("cls", "rep"), None),
        P(),
    )
    return jax.shard_map(
        functools.partial(per_device, mesh.shape["cls"], mesh.shape["rep"]),
        mesh=mesh,
        in_specs=placed,
        out_specs=(P("rep", "cls"), P("rep", "cls", None), P(("cls", "rep"), None)),
        check_vma=False,
    )
```

```python
import functools

import jax
import jax.numpy as jnp
from jax import lax
from jax.experimental import pallas as pl
from jax.experimental.pallas import tpu as pltpu
from jax.sharding import PartitionSpec as P

SLOTS = 8
NEG = -1e30
STATS = 128
PARTS = 4
PIECES = 8
NT = (((1,), (1,)), ((), ()))


def to_column(row, eye):
    return jnp.sum(jnp.where(eye, row, 0.0), axis=1, keepdims=True)


def to_row(col, eye):
    return jnp.sum(jnp.where(eye, col, 0.0), axis=0, keepdims=True)


def eye_of(n):
    shape = (n, n)
    return lax.broadcasted_iota(jnp.int32, shape, 0) == lax.broadcasted_iota(jnp.int32, shape, 1)


def each(count, step):
    if count <= 16:
        for i in range(count):
            step(i)
    else:
        lax.fori_loop(0, count, lambda i, carry: (step(i), carry)[1], 0)


def thirds(x):
    f32, bf16 = jnp.float32, jnp.bfloat16
    high = x.astype(bf16).astype(f32)
    rest = x - high
    mid = rest.astype(bf16).astype(f32)
    return high, mid, rest - mid


def step_kernel(
    n_cls,
    n_rep,
    slot_hbm,
    queries_hbm,
    positives_hbm,
    targets_hbm,
    gain_hbm,
    labels_hbm,
    features_hbm,
    weight_hbm,
    free_hbm,
    loss_ref,
    grads_ref,
    refreshed_ref,
    slot_ref,
    positives_ref,
    targets_ref,
    gain_ref,
    labels,
    turned_labels,
    features,
    weight,
    free,
    free_seats,
    seating,
    fresh_rows,
    fresh_seen,
    fresh_count,
    id_counts,
    q_slots,
    q_rows,
    out_rows,
    in_rows,
    logits,
    mixed,
    half_out,
    half_in,
    hits_out,
    hits_in,
    shares_out,
    shares_in,
    load_sem,
    q_sem,
    relay_sem,
    row_send,
    row_recv,
    half_sem,
    share_sem,
):
    f32, bf16 = jnp.float32, jnp.bfloat16
    cls = lax.axis_index("cls")
    rep = lax.axis_index("rep")
    partner = 1 - rep
    me = cls * n_rep + rep
    half_rows, width = features.shape
    padded = out_rows.shape[1]
    per_owner = half_rows // n_cls
    query_rows = q_slots.shape[1]
    n_query = q_rows.shape[0]
    own_half = n_query // n_rep
    usable, slot_rows = labels.shape[0], half_rows * n_rep
    lab_rows = usable * n_rep
    seats = n_cls * padded
    mine = rep * n_cls + cls
    span = n_cls // PARTS
    plane = cls // span
    inner = (plane > 0) & (plane < PARTS - 1)

    def seat_of(owner):
        return (owner ^ cls) * padded

    barrier = pltpu.get_barrier_semaphore()

    def greet(i):
        pl.semaphore_signal(barrier, inc=1, device_id=(cls ^ (n_cls - 1 - i), rep))

    each(n_cls - 1, greet)
    pl.semaphore_signal(barrier, inc=1, device_id=(cls, partner))

    chunks = usable // slot_rows
    pairs = [
        (features_hbm, features),
        (targets_hbm, targets_ref),
        (weight_hbm, weight),
        (gain_hbm, gain_ref),
        (queries_hbm.at[0], q_slots.at[mine]),
        (slot_hbm, slot_ref),
        (positives_hbm, positives_ref),
        (free_hbm, free),
    ]
    start = pl.multiple_of(rep * usable, slot_rows)
    pairs.append((labels_hbm.at[pl.ds(start, usable)], labels))
    loads = [pltpu.make_async_copy(a, b, load_sem.at[i]) for i, (a, b) in enumerate(pairs)]
    for copy in loads:
        copy.start()

    row_i = lax.broadcasted_iota(jnp.int32, (half_rows, half_rows), 0)
    col_i = lax.broadcasted_iota(jnp.int32, (half_rows, half_rows), 1)
    eye = row_i == col_i
    loads[1].wait()
    t_row = targets_ref[me].astype(f32)
    t_col = to_column(t_row, eye)
    rank = jnp.sum(jnp.where(t_col < t_row, 1.0, 0.0), axis=0, keepdims=True)
    owner = jnp.floor((rank + 0.5) * (1.0 / per_owner))
    seat_in = (rank - owner * per_owner).astype(jnp.int32)
    place = seat_of(owner.astype(jnp.int32)) + seat_in
    part_rows = span * padded

    def encode(low, high):
        rows = (high - low) * padded
        place_i = low * padded + lax.broadcasted_iota(jnp.int32, (rows, half_rows), 0)
        pick = jnp.where(place_i == place, 1.0, 0.0).astype(bf16)
        ordered = jnp.dot(pick, features[...], preferred_element_type=f32).astype(bf16)
        hidden = jnp.dot(ordered, weight[...], preferred_element_type=f32)
        scale = lax.rsqrt(jnp.mean(hidden * hidden, axis=1, keepdims=True) + 1e-06)
        encoded = hidden * scale * gain_ref[...].reshape(1, width)
        for k in range(low, high):
            out_rows[k] = encoded[(k - low) * padded : (k - low + 1) * padded].astype(bf16)

    loads[0].wait()
    loads[2].wait()
    loads[3].wait()
    encode(n_cls // 2, n_cls)
    loads[4].wait()

    pl.semaphore_wait(barrier, n_cls)

    def query_copy(k, slot, many):
        return pltpu.make_async_remote_copy(
            src_ref=q_slots.at[pl.ds(slot, many)],
            dst_ref=q_slots.at[pl.ds(slot, many)],
            send_sem=q_sem.at[0],
            recv_sem=q_sem.at[1],
            device_id=(cls ^ k, rep),
        )

    def row_copy(slot, many, part):
        return pltpu.make_async_remote_copy(
            src_ref=out_rows.at[pl.ds(slot, many)],
            dst_ref=in_rows.at[pl.ds(slot, many)],
            send_sem=row_send,
            recv_sem=row_recv.at[part],
            device_id=(cls ^ slot, rep),
        )

    def share_copy(k, source, slot, many):
        return pltpu.make_async_remote_copy(
            src_ref=shares_out.at[pl.ds(source, many)],
            dst_ref=shares_in.at[pl.ds(slot, many)],
            send_sem=share_sem.at[0],
            recv_sem=share_sem.at[1],
            device_id=(cls ^ k, rep),
        )

    def send_rows(part):
        top = (part + 1) * span - 1
        each(span if part else span - 1, lambda i: row_copy(top - i, 1, part).start())

    each(n_cls - 1, lambda i: query_copy(i + 1, mine, 1).start())
    pl.when(inner)(lambda: send_rows(2))
    encode(0, n_cls // 2)

    @pl.when(jnp.logical_not(inner))
    def _():
        query_copy(1, 0, n_cls - 1).wait_send()
        for part in (3, 2, 1, 0):
            send_rows(part)

    @pl.when(inner)
    def _():
        for part in (1, 0, 3):
            send_rows(part)

    in_rows[0] = out_rows[0]

    my_base = cls * slot_rows + rep * half_rows
    wanted = my_base.astype(f32) + row_i.astype(f32)

    def find(c, acc):
        t_c = targets_ref[c * n_rep + rep].astype(f32)
        return acc + jnp.where(t_c == wanted, (c + 1).astype(f32), 0.0)

    found = lax.fori_loop(0, n_cls, find, jnp.zeros((half_rows, half_rows), f32))
    src_col = jnp.sum(found, axis=1, keepdims=True) - 1.0
    src_row = to_row(src_col, eye)
    before = jnp.where((src_col == src_row) & (col_i < row_i), 1.0, 0.0)
    count_col = jnp.sum(before, axis=1, keepdims=True)
    seat_col = seat_of(src_col.astype(jnp.int32)) + count_col.astype(jnp.int32)
    seat_row = to_row(seat_col.astype(f32), eye).astype(jnp.int32)
    seat_i = lax.broadcasted_iota(jnp.int32, (half_rows, seats), 1)
    seating[...] = jnp.where(seat_i == seat_col, 1.0, 0.0).astype(bf16)
    turned_i = lax.broadcasted_iota(jnp.int32, (seats, half_rows), 0)
    turned = jnp.where(turned_i == seat_row, 1.0, 0.0).astype(bf16)
    loads[7].wait()
    free_seats[...] = jnp.dot(turned, free[...], preferred_element_type=f32)

    loads[5].wait()
    loads[6].wait()
    n_pos = positives_ref.shape[1]
    eye = eye_of(own_half)
    ids = []
    for p in range(n_pos):
        rows = [positives_ref[r, p : p + 1, :].astype(f32) for r in range(n_rep)]
        ids.append(jnp.concatenate([to_column(row, eye) for row in rows], axis=0).astype(jnp.int32))
    valid = jnp.zeros((n_query, 1), f32)
    for p in range(n_pos):
        valid = valid + jnp.where(ids[p] >= 0, 1.0, 0.0)
    id_counts[...] = jnp.broadcast_to(valid, id_counts.shape)
    slot_start = slot_ref[0] * slot_rows

    def counts_of(label):
        count = jnp.zeros((n_query, label.shape[1]), f32)
        for p in range(n_pos):
            count = count + jnp.where(ids[p] == label, 1.0, 0.0)
        return count

    fresh_base = cls * lab_rows + slot_start + rep * half_rows
    for part in range(PARTS):
        at_i = part * part_rows + lax.broadcasted_iota(jnp.int32, (half_rows, part_rows), 1)
        row_f = lax.broadcasted_iota(jnp.int32, (half_rows, part_rows), 0).astype(f32)
        at_row = jnp.sum(jnp.where(at_i == seat_col, row_f + 1.0, 0.0), axis=0, keepdims=True)
        fresh_seen[part] = at_row
        at_row = at_row.astype(jnp.int32)
        fresh_count[part] = counts_of(jnp.where(at_row > 0, fresh_base - 1 + at_row, -2))

    loads[8].wait()
    for k in range(chunks):
        at = slice(k * slot_rows, (k + 1) * slot_rows)
        turned_labels[:, at] = labels[at].T
    query_copy(1, 0, n_cls - 1).wait_recv()
    side = q_slots.at[pl.ds(rep * n_cls, n_cls)]
    relay = pltpu.make_async_remote_copy(
        src_ref=side,
        dst_ref=side,
        send_sem=relay_sem.at[0],
        recv_sem=relay_sem.at[1],
        device_id=(cls, partner),
    )
    relay.start()
    relay.wait_recv()
    for s in range(n_cls * n_rep):
        q_rows[s * query_rows : (s + 1) * query_rows] = q_slots[s].astype(f32)
    q = q_rows[...].astype(bf16)

    def split(power):
        high = power.astype(bf16)
        return high, (power - high.astype(f32)).astype(bf16)

    def sums(block, power, count):
        exp_sum = jnp.sum(power, axis=1, keepdims=True)
        pos_sum = jnp.sum(count * jnp.where(count > 0.0, block, 0.0), axis=1, keepdims=True)
        return exp_sum, pos_sum

    n = n_query
    peak = jnp.full((n, 1), NEG, f32)
    for k in range(chunks):
        at = slice(k * slot_rows, (k + 1) * slot_rows)
        block = jnp.dot(q, turned_labels[:, at], preferred_element_type=f32)
        fresh = slot_start == rep * usable + k * slot_rows
        block = jnp.where(fresh, NEG, block)
        logits[:, at] = block
        peak = jnp.maximum(peak, jnp.max(block, axis=1, keepdims=True))
    grad = jnp.zeros((n, width), f32)
    hits = jnp.zeros((n, width), f32)
    exp_sum = jnp.zeros((n, 1), f32)
    pos_sum = jnp.zeros((n, 1), f32)
    for k in range(chunks):
        at = slice(k * slot_rows, (k + 1) * slot_rows)
        first = cls * lab_rows + rep * usable + k * slot_rows
        fresh = slot_start == rep * usable + k * slot_rows
        label = first + lax.broadcasted_iota(jnp.int32, (n, slot_rows), 1)
        count = jnp.where(fresh, 0.0, counts_of(label))
        block = logits[:, at]
        power = jnp.exp(block - peak)
        mixed[0:n], mixed[n : 2 * n] = split(power)
        mixed[2 * n : 3 * n] = count.astype(bf16)
        out = jnp.dot(mixed[...], labels[at], preferred_element_type=f32)
        e, s = sums(block, power, count)
        grad = grad + (out[0:n] + out[n : 2 * n])
        hits, exp_sum, pos_sum = hits + out[2 * n : 3 * n], exp_sum + e, pos_sum + s

    second = jnp.where(inner, 2, 1)
    for turn, part in enumerate((0, second, jnp.where(inner, 1, 3), jnp.where(inner, 3, 2))):
        low = part * span + (0 if turn else 1)
        row_copy(low, span if turn else span - 1, part).wait_recv()
        at = pl.ds(pl.multiple_of(part * part_rows, 16), part_rows)
        landed = [in_rows[part * span + k].astype(f32) for k in range(span)]
        vectors = (free_seats[at] + jnp.concatenate(landed, axis=0)).astype(bf16)
        fresh_rows[at] = vectors
        block = lax.dot_general(q, vectors, NT, preferred_element_type=f32)
        block = jnp.where(fresh_seen[part] > 0.0, block, NEG)
        top = jnp.maximum(peak, jnp.max(block, axis=1, keepdims=True))
        power = jnp.exp(block - top)
        high, rest = split(power)
        count = fresh_count[part]
        out = jnp.dot(
            jnp.concatenate([high, rest, count.astype(bf16)], axis=0), vectors, preferred_element_type=f32
        )
        e, s = sums(block, power, count)
        a = jnp.exp(peak - top)
        grad = grad * a + (out[0:n] + out[n : 2 * n])
        hits, exp_sum, pos_sum = hits + out[2 * n : 3 * n], exp_sum * a + e, pos_sum + s
        peak = top

    lane = lax.broadcasted_iota(jnp.int32, (n, STATS), 1)
    stats = jnp.where(lane == 0, peak, jnp.where(lane == 1, exp_sum, pos_sum))

    def half(v, r):
        return jnp.where(r == 0, v[0:own_half], v[own_half:])

    half_out[:, 0:width] = half(grad, partner)
    half_out[:, width:] = half(stats, partner)
    hits_out[...] = half(hits, partner).astype(bf16)
    swaps = []
    for i, (a, b) in enumerate([(half_out, half_in), (hits_out, hits_in)]):
        swap = pltpu.make_async_remote_copy(
            src_ref=a,
            dst_ref=b,
            send_sem=half_sem.at[i],
            recv_sem=half_sem.at[2 + i],
            device_id=(cls, partner),
        )
        swap.start()
        swaps.append(swap)
    x = jnp.concatenate([half(grad, rep), half(stats, rep)], axis=1)
    xh = half(hits, rep)
    some = id_counts[pl.ds(pl.multiple_of(rep * own_half, own_half), own_half), :]
    for swap in swaps:
        swap.wait_recv()
    y, yh = half_in[...], hits_in[...].astype(f32)
    tiles = width // STATS

    def wide(v):
        return jnp.concatenate([v] * tiles, axis=1)

    def spread(v, i):
        return jnp.broadcast_to(v[:, width + i : width + i + 1], some.shape)

    xm, ym = spread(x, 0), spread(y, 0)
    m = jnp.maximum(xm, ym)
    a, b = jnp.exp(xm - m), jnp.exp(ym - m)
    exp_sum = spread(x, 1) * a + spread(y, 1) * b
    pos_sum = spread(x, 2) + spread(y, 2)
    hits = xh + yh
    inv = 1.0 / exp_sum
    term = x[:, 0:width] * wide(a * inv) + y[:, 0:width] * wide(b * inv) - hits * wide(1.0 / some)
    lane = lax.broadcasted_iota(jnp.int32, (own_half, STATS), 1)
    stats = jnp.zeros((own_half, STATS), f32)
    for i, value in enumerate([m, exp_sum, pos_sum]):
        for j, piece in enumerate(thirds(value)):
            stats = jnp.where(lane == 3 * j + i, piece, stats)
    term, hits, stats = term.astype(bf16), hits.astype(bf16), stats.astype(bf16)
    for c in range(n_cls):
        at = slice(c * query_rows, (c + 1) * query_rows)
        shares_out[c, :, 0:width] = term[at]
        shares_out[c, :, width : 2 * width] = hits[at]
        shares_out[c, :, 2 * width :] = stats[at]

    def send_share(i):
        other = i + (cls <= i).astype(jnp.int32)
        share_copy(cls ^ other, other, cls ^ other, 1).start()

    each(n_cls - 1, send_share)
    shares_in[0] = shares_out[cls]

    refreshed = jnp.dot(seating[...], fresh_rows[...], preferred_element_type=f32)
    refreshed_ref[...] = refreshed.astype(bf16)
    pl.when(inner)(lambda: query_copy(1, 0, n_cls - 1).wait_send())
    row_copy(1, n_cls - 1, 0).wait_send()
    relay.wait_send()
    for swap in swaps:
        swap.wait_send()
    id_count = id_counts[pl.ds(mine * query_rows, query_rows), :][:, 0:1]

    share_copy(1, 0, 1, n_cls - 1).wait_recv()
    stats = jnp.concatenate([shares_in[k, :, 2 * width :].astype(f32) for k in range(n_cls)], axis=0)

    def gather(i):
        parts = [jnp.broadcast_to(stats[:, 3 * j + i : 3 * j + i + 1], stats.shape) for j in range(3)]
        whole = parts[0] + parts[1] + parts[2]
        return [whole[k * query_rows : (k + 1) * query_rows] for k in range(n_cls)]

    ms, es, ps = gather(0), gather(1), gather(2)
    m = functools.reduce(jnp.maximum, ms)
    es = [e * jnp.exp(x - m) for e, x in zip(es, ms)]
    exp_sum = functools.reduce(jnp.add, es)
    pos_sum = functools.reduce(jnp.add, ps)
    inv, inv_count = 1.0 / exp_sum, 1.0 / id_count
    grad = jnp.zeros((query_rows, width), f32)
    for k in range(n_cls):
        rho = es[k] * inv
        back = (rho - 1.0) * inv_count
        grad = grad + wide(rho) * shares_in[k, :, 0:width].astype(f32)
        grad = grad + wide(back) * shares_in[k, :, width : 2 * width].astype(f32)
    loss = (m + jnp.log(exp_sum))[:, 0:1] - pos_sum[:, 0:1] * inv_count
    loss_ref[...] = to_row(loss, eye_of(query_rows))
    grads_ref[0] = grad.astype(bf16)
    share_copy(1, 0, 1, n_cls - 1).wait_send()


def pass_on(loss, grads, refreshed, loss_hbm, grads_hbm, refreshed_hbm, sem):
    rows = refreshed.shape[0] // PIECES
    for i in range(PIECES):
        at = pl.ds(i * rows, rows)
        pltpu.make_async_copy(refreshed.at[at], refreshed_hbm.at[at], sem.at[2]).start()
    small = [
        pltpu.make_async_copy(loss, loss_hbm, sem.at[0]),
        pltpu.make_async_copy(grads, grads_hbm, sem.at[1]),
    ]
    for copy in small:
        copy.start()
    for copy in small:
        copy.wait()
    pltpu.make_async_copy(refreshed, refreshed_hbm, sem.at[2]).wait()


def per_device(
    n_cls,
    n_rep,
    queries,
    positives,
    label_vectors,
    refresh_slot,
    features,
    encoder_weight,
    encoder_gain,
    free_vectors,
    targets,
):
    f32, bf16 = jnp.float32, jnp.bfloat16
    total = n_cls * n_rep
    lab_rows, width = label_vectors.shape
    usable = lab_rows // n_rep
    slot_rows = lab_rows // SLOTS
    half_rows = slot_rows // n_rep
    per_owner = half_rows // n_cls
    padded = -(-per_owner // 8) * 8
    query_rows = queries.shape[1]
    n_query = total * query_rows
    own_half = n_query // n_rep
    n_pos = positives.shape[2]
    share = 2 * width + STATS
    vmem = pl.BlockSpec(memory_space=pltpu.VMEM)
    hbm = pl.BlockSpec(memory_space=pltpu.HBM)
    dma = pltpu.SemaphoreType.DMA
    outs = (
        ((1, query_rows), f32),
        ((1, query_rows, width), bf16),
        ((half_rows, width), bf16),
    )
    results = pl.pallas_call(
        functools.partial(step_kernel, n_cls, n_rep),
        out_shape=tuple(pltpu.VMEM(*out) for out in outs),
        in_specs=[hbm] * 9,
        out_specs=(vmem,) * 3,
        scratch_shapes=[
            pltpu.SMEM((1,), jnp.int32),
            pltpu.VMEM((n_rep, n_pos, own_half), jnp.int32),
            pltpu.VMEM((total, 1, half_rows), jnp.int32),
            pltpu.VMEM((width,), f32),
            pltpu.VMEM((usable, width), bf16),
            pltpu.VMEM((width, usable), bf16),
            pltpu.VMEM((half_rows, width), bf16),
            pltpu.VMEM((width, width), bf16),
            pltpu.VMEM((half_rows, width), bf16),
            pltpu.VMEM((n_cls * padded, width), f32),
            pltpu.VMEM((half_rows, n_cls * padded), bf16),
            pltpu.VMEM((n_cls * padded, width), bf16),
            pltpu.VMEM((PARTS, 1, n_cls // PARTS * padded), f32),
            pltpu.VMEM((PARTS, n_query, n_cls // PARTS * padded), f32),
            pltpu.VMEM((n_query, STATS), f32),
            pltpu.VMEM((total, query_rows, width), bf16),
            pltpu.VMEM((n_query, width), f32),
            pltpu.VMEM((n_cls, padded, width), bf16),
            pltpu.VMEM((n_cls, padded, width), bf16),
            pltpu.VMEM((n_query, usable), f32),
            pltpu.VMEM((3 * n_query, slot_rows), bf16),
            pltpu.VMEM((own_half, width + STATS), f32),
            pltpu.VMEM((own_half, width + STATS), f32),
            pltpu.VMEM((own_half, width), bf16),
            pltpu.VMEM((own_half, width), bf16),
            pltpu.VMEM((n_cls, query_rows, share), bf16),
            pltpu.VMEM((n_cls, query_rows, share), bf16),
            dma((9,)),
            dma((2,)),
            dma((2,)),
            dma,
            dma((PARTS,)),
            dma((4,)),
            dma((2,)),
        ],
        compiler_params=pltpu.CompilerParams(
            collective_id=0, has_side_effects=True, vmem_limit_bytes=48 * 2**20
        ),
    )(
        refresh_slot.reshape(1),
        *[
            pltpu.with_memory_space_constraint(x, pltpu.HBM)
            for x in (
                queries,
                positives.transpose(0, 2, 1),
                targets.reshape(total, 1, half_rows),
                encoder_gain,
                label_vectors,
                features,
                encoder_weight,
                free_vectors,
            )
        ]
    )
    return pl.pallas_call(
        pass_on,
        out_shape=tuple(jax.ShapeDtypeStruct(*out) for out in outs),
        in_specs=[vmem] * 3,
        out_specs=(hbm,) * 3,
        scratch_shapes=[dma((3,))],
    )(*[pltpu.with_memory_space_constraint(x, pltpu.VMEM) for x in results])


def solution(mesh):
    placed = (
        P("rep", "cls", None),
        P(),
        P("cls", None),
        P(),
        P(("cls", "rep"), None),
        P(),
        P(),
        P(("cls", "rep"), None),
        P(),
    )
    return jax.shard_map(
        functools.partial(per_device, mesh.shape["cls"], mesh.shape["rep"]),
        mesh=mesh,
        in_specs=placed,
        out_specs=(P("rep", "cls"), P("rep", "cls", None), P(("cls", "rep"), None)),
        check_vma=False,
    )
```
